32 devices in a mesh: rep: 8 (over y, x, core), tp: 4 (over z).
Axes of the slice: x: 2, y: 2, z: 4, core: 2. Of those that a mesh axis runs over, the one named last changes fastest.
Arguments:
- tokens: bfloat16 [8192, 1280], P(('rep', 'tp')), may hold values from -6 to 6
- view_ids: int32 [32, 4], P('rep'), may hold values from 0 to 31
- time_ids: int32 [32], P('rep'), may hold values from 0 to 999
- camera_table: float32 [32, 1280], replicated, may hold values from -6 to 6
- norm_attn: float32 [2, 1280], replicated, may hold values from 0.1 to 1.9
- norm_ffn: float32 [2, 1280], replicated, may hold values from 0.1 to 1.9
- w_query: bfloat16 [2, 1280, 1280], P(None, ('rep', 'tp')), may hold values from -0.1677051 to 0.1677051
- w_key: bfloat16 [2, 1280, 1280], P(None, ('rep', 'tp')), may hold values from -6.764106 to 6.764106
- w_value: bfloat16 [2, 1280, 1280], P(None, ('rep', 'tp')), may hold values from -0.15625 to 0.15625
- w_out: bfloat16 [2, 1280, 1280], P(None, ('rep', 'tp')), may hold values from -0.15625 to 0.15625
- w_gate: bfloat16 [2, 1280, 5120], P(None, ('rep', 'tp')), may hold values from -0.15625 to 0.15625
- w_up: bfloat16 [2, 1280, 5120], P(None, ('rep', 'tp')), may hold values from -0.15625 to 0.15625
- w_down: bfloat16 [2, 1280, 5120], P(None, ('rep', 'tp')), may hold values from -0.078125 to 0.078125
Outputs:
- denoised: bfloat16 [8192, 1280], P(('rep', 'tp'))
The draws below stay inside these ranges and needn't reach their ends.
All inputs are finite; a program needn't handle non-finite values.
Results may differ from the reference program's by a relative error of at most 0.035.
Values may be sent and summed in bfloat16 or wider, within the bound.
A program may use at most 128 MiB of HBM per device.

```python
import math
import jax
import jax.numpy as jnp
from jax import lax

D = 1280
FF = 5120
HEADS = 8
VIEWS = 4
HW = 64
LAYERS = 2
NPOSE = 32
CAMS = 32
ROWS = 8192
N_TP = 4


def query_base(key):
    base = jax.random.normal(jax.random.fold_in(key, 11), (LAYERS, D, D), jnp.float32)
    return jnp.clip(base, -6.0, 6.0) * D ** (-0.5)


def draw_w_query(key, part):
    return query_base(key).astype(jnp.bfloat16)


def draw_w_key(key, part):
    other = jax.random.normal(jax.random.fold_in(key, 12), (LAYERS, D, D), jnp.float32)
    other = jnp.clip(other, -6.0, 6.0) * D ** (-0.5)
    return other.astype(jnp.bfloat16)


def touch_ends(drawn, own_key, low, high):
    dims = drawn.shape
    spot = [jax.random.randint(jax.random.fold_in(own_key, axis), (), 0, dims[axis]) for axis in range(len(dims))]
    drawn = drawn.at[tuple(spot)].set(low)
    longest = dims.index(max(dims))
    spot[longest] = (spot[longest] + 1) % dims[longest]
    return drawn.at[tuple(spot)].set(high)


def block_scale(rng, dims, shards, smallest, top_value):
    loudness = 1.0
    for dim, parts in shards:
        draws = jax.random.uniform(jax.random.fold_in(jax.random.fold_in(rng, 6), dim), (parts,), jnp.float32, smallest / len(shards), top_value / len(shards))
        loudness = loudness * jnp.repeat(jnp.exp(draws), dims[dim] // parts).reshape((-1,) + (1,) * (len(dims) - 1 - dim))
    return loudness


def gaussian(key, shape, scale, limit, shards=(), kind=jnp.bfloat16):
    values = jax.random.normal(key, shape, jnp.float32) * scale
    if len(shards) > 0:
        values = block_scale(key, shape, shards, -0.22, 0.18) * values
    return jnp.clip(values, min=-limit, max=limit).astype(kind)


def setup_inputs(seed: int = 0) -> dict:
    streams_of = jax.random.split(jax.random.key(seed), 14)
    tokens = gaussian(streams_of[0], (ROWS, D), 1.0, 6.0, ((0, 32),))
    view_ids = touch_ends(jax.random.randint(streams_of[1], (CAMS, VIEWS), 0, NPOSE), jax.random.fold_in(streams_of[1], 1), 0, NPOSE - 1).astype(jnp.int32)
    time_ids = touch_ends(jax.random.randint(streams_of[2], (CAMS,), 0, 1000), jax.random.fold_in(streams_of[2], 1), 0, 999).astype(jnp.int32)
    camera_table = gaussian(streams_of[3], (NPOSE, D), 1.0, 6.0, (), jnp.float32)
    norm_attn = jnp.clip(1.0 + 0.18 * jax.random.normal(streams_of[4], (LAYERS, D), jnp.float32), 0.1, 1.9)
    norm_ffn = jnp.clip(1.0 + 0.18 * jax.random.normal(streams_of[5], (LAYERS, D), jnp.float32), 0.1, 1.9)
    w_query = draw_w_query(jax.random.fold_in(streams_of[13], 71), 0)
    w_key = draw_w_key(jax.random.fold_in(streams_of[13], 71), 0)
    w_value = gaussian(streams_of[8], (LAYERS, D, D), D ** -0.5, 0.15625, ((1, 32),))
    w_out = gaussian(streams_of[9], (LAYERS, D, D), D ** -0.5, 0.15625, ((1, 32),))
    w_gate = gaussian(streams_of[10], (LAYERS, D, FF), D ** -0.5, 0.15625, ((1, 32),))
    w_up = gaussian(streams_of[11], (LAYERS, D, FF), D ** -0.5, 0.15625, ((1, 32),))
    w_down = gaussian(streams_of[12], (LAYERS, D, FF), FF ** -0.5, 0.078125, ((1, 32),))
    return dict(tokens=tokens, view_ids=view_ids, time_ids=time_ids, camera_table=camera_table, norm_attn=norm_attn, norm_ffn=norm_ffn, w_query=w_query, w_key=w_key, w_value=w_value, w_out=w_out, w_gate=w_gate, w_up=w_up, w_down=w_down)


def layer_norm(activations, gain_vector):
    average = lax.optimization_barrier(jnp.mean(activations, axis=-1, keepdims=True))
    centred = activations - average
    spread = lax.optimization_barrier(jnp.mean(centred * centred, axis=-1, keepdims=True))
    return (centred * lax.rsqrt(spread + 1e-05) * gain_vector).astype(jnp.bfloat16)

def time_code(step_ids, width):
    half_width = width // 2
    frequency = jnp.exp(-math.log(10000.0) * jnp.arange(half_width, dtype=jnp.float32) / half_width)
    angles = step_ids.astype(jnp.float32)[:, None] * frequency[None, :]
    return jnp.concatenate([jnp.cos(angles), jnp.sin(angles)], axis=1)

def split_sum(mixed_rows, weight):
    row_count = mixed_rows.shape[0]
    inner_width = mixed_rows.shape[1] // N_TP
    left_side = mixed_rows.astype(jnp.float32).reshape(row_count, N_TP, inner_width)
    right_side = weight.astype(jnp.float32).reshape(weight.shape[0], N_TP, inner_width)
    term_rows = jnp.einsum('snc,onc->nso', left_side, right_side).astype(jnp.bfloat16)
    term_rows = lax.optimization_barrier(term_rows)
    return lax.optimization_barrier(jnp.sum(term_rows.astype(jnp.float32), axis=0))

def attention(query_rows, key_rows, value_rows):
    seq_len = query_rows.shape[0]
    head_size = D // HEADS
    query_heads = query_rows.astype(jnp.float32).reshape(seq_len, HEADS, head_size)
    key_heads = key_rows.astype(jnp.float32).reshape(seq_len, HEADS, head_size)
    value_heads = value_rows.astype(jnp.float32).reshape(seq_len, HEADS, head_size)
    scores = jnp.einsum('qhd,khd->hqk', query_heads, key_heads) * head_size ** (-0.5)
    peak = lax.optimization_barrier(jnp.max(scores, axis=-1, keepdims=True))
    expons = jnp.exp(scores - peak)
    attn_probs = (expons / lax.optimization_barrier(jnp.sum(expons, axis=-1, keepdims=True))).astype(jnp.bfloat16)
    mixed_rows = jnp.einsum('hqk,khd->qhd', attn_probs.astype(jnp.float32), value_heads)
    return mixed_rows.astype(jnp.bfloat16).reshape(seq_len, D)

def reference(tokens, view_ids, time_ids, camera_table, norm_attn, norm_ffn, w_query, w_key, w_value, w_out, w_gate, w_up, w_down):
    seq_len = VIEWS * HW
    set_count = tokens.shape[0] // seq_len
    blocks = tokens.reshape(set_count, seq_len, D)

    def one_set(packed):
        block, views_here, step_here = packed
        camera = jnp.repeat(camera_table[views_here], HW, axis=0)
        stream = block.astype(jnp.float32) + camera + time_code(step_here[None], D)
        for layer_index in range(LAYERS):
            normed = layer_norm(stream, norm_attn[layer_index])
            query_rows = jnp.dot(normed, w_query[layer_index], preferred_element_type=jnp.float32).astype(jnp.bfloat16)
            key_rows = jnp.dot(normed, w_key[layer_index], preferred_element_type=jnp.float32).astype(jnp.bfloat16)
            value_rows = jnp.dot(normed, w_value[layer_index], preferred_element_type=jnp.float32).astype(jnp.bfloat16)
            mixed_rows = attention(query_rows, key_rows, value_rows)
            stream = stream + split_sum(mixed_rows, w_out[layer_index])
            normed = layer_norm(stream, norm_ffn[layer_index])
            gate_part = jnp.dot(normed, w_gate[layer_index], preferred_element_type=jnp.float32)
            up_part = jnp.dot(normed, w_up[layer_index], preferred_element_type=jnp.float32)
            hidden = (jax.nn.gelu(gate_part, approximate=False) * up_part).astype(jnp.bfloat16)
            stream = stream + split_sum(hidden, w_down[layer_index])
        return stream.astype(jnp.bfloat16)
    result = lax.map(one_set, (blocks, view_ids, time_ids))
    return result.reshape(tokens.shape[0], D)
```

```python
import functools
import math

import jax
import jax.numpy as jnp
from jax import lax
from jax.experimental import pallas as pl
from jax.experimental.pallas import tpu as pltpu
from jax.sharding import PartitionSpec as P

D = 1280
HEADS = 8
VIEWS = 4
HW = 64
LAYERS = 2


def layer_norm(activations, gain_vector):
    average = jnp.mean(activations, axis=-1, keepdims=True)
    centred = activations - average
    spread = jnp.mean(centred * centred, axis=-1, keepdims=True)
    return (centred * lax.rsqrt(spread + 1e-05) * gain_vector).astype(jnp.bfloat16)


def time_code(step_ids, width):
    half_width = width // 2
    frequency = jnp.exp(-math.log(10000.0) * jnp.arange(half_width, dtype=jnp.float32) / half_width)
    angles = step_ids.astype(jnp.float32)[:, None] * frequency[None, :]
    return jnp.concatenate([jnp.cos(angles), jnp.sin(angles)], axis=1)


def conditioning(row_ids, view_ids, time_ids, camera_table):
    set_ids = row_ids // (VIEWS * HW)
    slot_ids = set_ids * VIEWS + row_ids // HW % VIEWS
    flat_views = view_ids.reshape(-1)
    slot_range = jnp.arange(flat_views.shape[0], dtype=jnp.int32)
    pose_ids = jnp.sum(
        jnp.where(slot_ids[:, None] == slot_range[None, :], flat_views[None, :], 0), axis=1
    )
    set_range = jnp.arange(time_ids.shape[0], dtype=jnp.int32)
    step_ids = jnp.sum(
        jnp.where(set_ids[:, None] == set_range[None, :], time_ids[None, :], 0), axis=1
    )
    pose_range = jnp.arange(camera_table.shape[0], dtype=jnp.int32)
    onehot_pose = (pose_ids[:, None] == pose_range[None, :]).astype(jnp.float32)
    camera = jnp.dot(onehot_pose, camera_table, precision=lax.Precision.HIGHEST)
    return camera + time_code(step_ids, camera_table.shape[1])


MESH = pl.DeviceIdType.MESH
LANES = 128
PLANE = 4


class Pieces:
    def __init__(self, chips_z, layers, tile_count, send_sems):
        self.chips_z, self.layers, self.tile_count = chips_z, layers, tile_count
        self.send_sems = send_sems
        self.used = 0
        self.finish = []
        rep_here = lax.axis_index("rep")
        self.z = lax.axis_index("tp")
        self.q = rep_here // 2
        self.core = rep_here % 2
        flip_x = self.q + 1 - 2 * (self.q % 2)
        flip_y = (self.q + 2) % PLANE
        self.first = flip_x + self.core * (flip_y - flip_x)
        self.second = flip_y + self.core * (flip_x - flip_y)
        self.diagonal = PLANE - 1 - self.q

    def at(self, q, core, z):
        return (q * 2 + core, z)

    def sibling(self):
        return self.at(self.q, 1 - self.core, self.z)

    def peer(self, q):
        return self.at(q, self.core, self.z)

    def line(self, step):
        return self.at(self.q, self.core, self.z + step)

    def copy(self, source, target, arrived, device, condition=None, later=True):
        one = pltpu.make_async_remote_copy(
            src_ref=source,
            dst_ref=target,
            send_sem=self.send_sems.at[self.used],
            recv_sem=arrived,
            device_id=device,
            device_id_type=MESH,
        )
        self.used += 1
        if later:
            self.finish.append((condition, one))
        return one

    def arrival(self, region, arrived):
        pltpu.make_async_remote_copy(
            src_ref=region,
            dst_ref=region,
            send_sem=self.send_sems.at[0],
            recv_sem=arrived,
            device_id=self.sibling(),
            device_id_type=MESH,
        ).wait_recv()


def both(first, second):
    if first is None or second is None:
        return second if first is None else first
    return jnp.logical_and(first, second)


def guarded(condition, action):
    if condition is None:
        action()
    else:
        pl.when(condition)(action)


def fused_kernel(
    shape,
    tokens_ref,
    cond_ref,
    gain_attn_ref,
    gain_ffn_ref,
    wq_ref,
    wk_ref,
    wv_ref,
    wo_ref,
    wg_ref,
    wu_ref,
    wd_ref,
    out_ref,
    full,
    normed,
    landing,
    staging,
    total,
    stream,
    own_sems,
    send_sems,
    line_sems,
    plane_sems,
    share_sems,
    pair_attn_sems,
    pair_ffn_sems,
    rows_sems,
    term_sems,
):
    layers, chips_z, width, tile, tile_count, head_size = shape
    net = Pieces(chips_z, layers, tile_count, send_sems)
    z, q, core = net.z, net.q, net.core
    rows = stream.shape[0]
    here = core * chips_z + z

    def attn_piece(layer, q_from, core_from, z_from):
        return full.at[layer, 0:4, q_from, core_from * chips_z + z_from]

    def ffn_piece(layer, part, core_from, z_from):
        return full.at[
            layer, 4:7, :, core_from * chips_z + z_from, :, pl.ds(part * tile, tile)
        ]

    def in_line(offset):
        if offset == 0:
            return None
        return z + offset < chips_z if offset > 0 else z + offset >= 0

    def beyond(step):
        return z < chips_z - 1 if step > 0 else z > 0

    own = []
    for layer in range(layers):
        group = []
        for kind, ref in enumerate((wq_ref, wk_ref, wv_ref, wo_ref)):
            group.append((ref.at[layer], full.at[layer, kind, q, here]))
        own.append(group)
    for layer in range(layers):
        group = []
        for kind, ref in enumerate((wg_ref, wu_ref, wd_ref)):
            group.append(
                (ref.at[layer, :, pl.ds(q * width, width)], full.at[layer, 4 + kind, q, here])
            )
        own.append(group)
    local, slot = [], 0
    for group in own:
        copies = []
        for source, target in group:
            copies.append(pltpu.make_async_copy(source, target, own_sems.at[slot]))
            copies[-1].start()
            slot += 1
        local.append(copies)

    def wait_local(index):
        for one in local[index]:
            one.wait()

    barrier = pltpu.get_barrier_semaphore()
    for device in (
        net.sibling(),
        net.peer(net.first),
        net.peer(net.second),
        net.peer(net.diagonal),
    ):
        pl.semaphore_signal(barrier, inc=1, device_id=device, device_id_type=MESH)
    for step in (1, -1):
        def greet(step=step):
            pl.semaphore_signal(barrier, inc=1, device_id=net.line(step), device_id_type=MESH)
        pl.when(beyond(step))(greet)
    count = jnp.int32(4) + (z > 0).astype(jnp.int32) + (z < chips_z - 1).astype(jnp.int32)
    pl.semaphore_wait(barrier, count)

    def along_line(stage, region, pair_sem, offset):
        z_from = z + offset
        valid = in_line(offset)
        sends = []
        for step in (1, -1):
            if offset == 0 or (offset > 0) == (step < 0):
                ahead = beyond(step)
                one = net.copy(
                    region,
                    region,
                    line_sems.at[stage, z_from],
                    net.line(step),
                    both(valid, ahead),
                )
                sends.append((ahead, one))
        share = net.copy(region, region, pair_sem, net.sibling(), valid)

        def action():
            if offset:
                net.arrival(region, line_sems.at[stage, z_from])
            for ahead, one in sends:
                guarded(ahead, one.start)
            share.start()

        guarded(valid, action)

    def attn_line(layer, offset):
        along_line(
            layer,
            attn_piece(layer, q, core, z + offset),
            pair_attn_sems.at[layer, q, z + offset],
            offset,
        )

    def attn_plane(layer, offset):
        z_from = z + offset
        valid = in_line(offset)
        region = attn_piece(layer, q, core, z_from)
        sends = [
            net.copy(region, region, plane_sems.at[layer, q, z_from], net.peer(peer), valid)
            for peer in (net.first, net.second)
        ]

        def action():
            for one in sends:
                one.start()

        guarded(valid, action)

    def from_plane(layer, offset, which):
        z_from = z + offset
        valid = in_line(offset)
        peer = (net.first, net.second, net.diagonal)[which]
        region = attn_piece(layer, peer, core, z_from)
        arrived = plane_sems.at[layer, peer, z_from]
        sends = []
        if which == 0:
            sends.append(net.copy(region, region, arrived, net.peer(net.second), valid))
        sends.append(
            net.copy(
                region, region, pair_attn_sems.at[layer, peer, z_from], net.sibling(), valid
            )
        )

        def action():
            net.arrival(region, arrived)
            for one in sends:
                one.start()

        guarded(valid, action)

    def attn_pairs(layer):
        def wait_one(index, carry):
            q_from, z_from = index // chips_z, index % chips_z
            net.arrival(
                attn_piece(layer, q_from, 1 - core, z_from),
                pair_attn_sems.at[layer, q_from, z_from],
            )
            return carry

        lax.fori_loop(0, PLANE * chips_z, wait_one, 0)

    def exchange_columns(layer):
        for peer in (net.first, net.second, net.diagonal):
            for kind, ref in enumerate((wg_ref, wu_ref, wd_ref)):
                net.copy(
                    ref.at[layer, :, pl.ds(peer * width, width)],
                    full.at[layer, 4 + kind, q, here],
                    share_sems.at[layer, q],
                    net.peer(peer),
                ).start()

    def columns_here(layer):
        wait_local(layers + layer)
        for peer in (net.first, net.second, net.diagonal):
            net.arrival(full.at[layer, 4:7, peer, here], share_sems.at[layer, peer])

    def ffn_line(layer, part, offset):
        along_line(
            layers + layer * tile_count + part,
            ffn_piece(layer, part, core, z + offset),
            pair_ffn_sems.at[layer * tile_count + part, z + offset],
            offset,
        )

    def ffn_pairs(layer, part):
        for z_from in range(chips_z):
            net.arrival(
                ffn_piece(layer, part, 1 - core, z_from),
                pair_ffn_sems.at[layer * tile_count + part, z_from],
            )

    def offsets(hops):
        return [hops, -hops] if hops else [0]

    steps = []
    for layer in range(layers):
        steps.append(("attn", layer, 0))
    for layer in range(layers):
        for part in range(tile_count):
            steps.append(("ffn", layer, part))

    def send_own(step):
        kind, layer, part = step
        if kind == "attn":
            wait_local(layer)
            attn_line(layer, 0)
        else:
            if part == 0:
                columns_here(layer)
            ffn_line(layer, part, 0)

    def pass_on(step, hops):
        kind, layer, part = step
        for offset in offsets(hops):
            if kind == "attn":
                attn_line(layer, offset)
            else:
                ffn_line(layer, part, offset)

    queue = []
    for index, step in enumerate(steps):
        if index == 0:
            queue.append((step, 0))
        for hops in range(1, chips_z):
            if hops == 2 and index + 1 < len(steps):
                queue.append((steps[index + 1], 0))
            queue.append((step, hops))
    done = [0]

    def pump(amount):
        for _ in range(amount):
            if done[0] < len(queue):
                step, hops = queue[done[0]]
                done[0] += 1
                if hops == 0:
                    send_own(step)
                else:
                    pass_on(step, hops)

    def pump_until(step):
        while (step, chips_z - 1) in queue[done[0] :]:
            pump(1)

    plane_queue = []
    for layer in range(layers):
        items = []
        for hops in range(chips_z):
            items.append((2 * hops, "out", layer, hops))
            items.append((2 * hops + 1, "near", layer, hops))
            items.append((2 * hops + 2.5, "far", layer, hops))
        items.sort(key=lambda item: item[0])
        plane_queue.append(items)
    plane_done = [0] * layers

    def spread(layer, amount):
        for _ in range(amount):
            if plane_done[layer] == len(plane_queue[layer]):
                return
            _, what, _, hops = plane_queue[layer][plane_done[layer]]
            plane_done[layer] += 1
            for offset in offsets(hops):
                if what == "out":
                    attn_plane(layer, offset)
                elif what == "near":
                    from_plane(layer, offset, 0)
                    from_plane(layer, offset, 1)
                else:
                    from_plane(layer, offset, 2)

    chunk = 64 if rows % 64 == 0 else rows

    def normalise(gain_ref, layer):
        def one(index, carry):
            span = pl.ds(pl.multiple_of(index * chunk, chunk), chunk)
            normed[0, span, :] = layer_norm(stream[span, :], gain_ref[layer : layer + 1, :])
            return carry

        lax.fori_loop(0, rows // chunk, one, 0)

    def weight(layer, kind, index, size):
        span = pl.ds(pl.multiple_of(index * size, size), size)
        return full[layer, kind, :, :, :, span].reshape(width, size)

    column = 256 if width % 256 == 0 else LANES

    def project(layer, kind):
        def one(index, carry):
            span = pl.ds(pl.multiple_of(index * column, column), column)
            staging[kind, :, span] = jnp.dot(
                normed[0], weight(layer, kind, index, column), preferred_element_type=jnp.float32
            ).astype(jnp.bfloat16)
            return carry

        lax.fori_loop(0, width // column, one, 0)

    window = head_window(head_size)

    def attend_heads(first_head, last_head):
        def one(head, carry):
            start = head * head_size
            base = pl.multiple_of(start // LANES * LANES, LANES)
            span = pl.ds(base, window)
            lane = lax.broadcasted_iota(jnp.int32, (1, window), 1) + base
            inside = jnp.logical_and(lane >= start, lane < start + head_size)
            query = staging[0, :, span]
            scores = out_terms(
                jnp.where(inside, query, jnp.zeros_like(query)), staging[1, :, span]
            ) * head_size ** (-0.5)
            peak = jnp.max(scores, axis=-1, keepdims=True)
            expons = jnp.exp(scores - peak)
            probs = (expons / jnp.sum(expons, axis=-1, keepdims=True)).astype(jnp.bfloat16)
            mixed = jnp.dot(
                probs, staging[2, :, span], preferred_element_type=jnp.float32
            ).astype(jnp.bfloat16)
            staging[0, :, span] = jnp.where(inside, mixed, query)
            return carry

        lax.fori_loop(first_head, last_head, one, 0)

    def project_out(layer):
        def one(index, carry):
            span = pl.ds(pl.multiple_of(index * column, column), column)
            stream[...] += out_terms(staging[0, :, span], weight(layer, 3, index, column))
            return carry

        lax.fori_loop(0, width // column, one, 0)

    def ffn_tile(layer, part, place):
        gate = jnp.dot(
            normed[place], weight(layer, 4, part, tile), preferred_element_type=jnp.float32
        )
        up = jnp.dot(
            normed[place], weight(layer, 5, part, tile), preferred_element_type=jnp.float32
        )
        gate = 0.5 * gate * (1.0 + lax.erf(gate * math.sqrt(0.5)))
        hidden = (gate * up).astype(jnp.bfloat16)
        term = out_terms(hidden, weight(layer, 6, part, tile))
        if part == 0:
            total[place] = term
        else:
            total[place] = total[place] + term

    pump(1)
    spread(0, 1)
    exchange_columns(0)
    views = cond_ref.shape[0]
    per_view = rows // views
    for view in range(views):
        span = pl.ds(view * per_view, per_view)
        stream[span, :] = tokens_ref[span, :].astype(jnp.float32) + cond_ref[view : view + 1, :]
    normalise(gain_attn_ref, 0)

    pump(1)
    spread(0, 1)
    pump(2)
    spread(0, 2)
    spread(0, 1)
    pump(1)
    spread(0, 2)
    pump(1)
    spread(0, 2)
    pump(1)
    spread(0, 20)
    pump(1)
    attn_pairs(0)

    for layer in range(layers):
        last_layer = layer == layers - 1
        if layer:
            pump_until(("attn", layer, 0))
            spread(layer, 20)
            attn_pairs(layer)
            normalise(gain_attn_ref, layer)
        project(layer, 0)
        project(layer, 1)
        project(layer, 2)
        pump(1)
        if not last_layer:
            pump_until(("attn", layer + 1, 0))
            exchange_columns(layer + 1)
            spread(layer + 1, 3)
        attend_heads(0, D // head_size)
        pump(1)
        project_out(layer)
        normalise(gain_ffn_ref, layer)

        rows_sent = [
            net.copy(
                normed.at[0],
                normed.at[1 + side],
                rows_sems.at[layer, side],
                net.peer((net.first, net.second)[side]),
                later=False,
            )
            for side in range(2)
        ]
        for one in rows_sent:
            one.start()
        pump(2)
        net.arrival(normed.at[1], rows_sems.at[layer, 0])
        rows_sent.append(
            net.copy(
                normed.at[1],
                normed.at[3],
                rows_sems.at[layer, 2],
                net.peer(net.second),
                later=False,
            )
        )
        rows_sent[-1].start()
        if not last_layer:
            spread(layer + 1, 3)
        pump(1)
        net.arrival(normed.at[2], rows_sems.at[layer, 1])
        pump(1)

        for part in range(tile_count - 1):
            pump_until(("ffn", layer, part))
            ffn_pairs(layer, part)
            if part == 0:
                net.arrival(normed.at[3], rows_sems.at[layer, 2])

            def one(place, carry, part=part):
                ffn_tile(layer, part, place)
                return carry

            lax.fori_loop(0, PLANE, one, 0)
        for sent in rows_sent:
            sent.wait_send()
        part = tile_count - 1
        pump_until(("ffn", layer, part))
        ffn_pairs(layer, part)

        terms_sent = []

        def send_term(slot, target, arrived, peer):
            terms_sent.append(
                net.copy(
                    staging.at[slot], landing.at[target], arrived, net.peer(peer), later=False
                )
            )
            terms_sent[-1].start()

        ffn_tile(layer, part, 3)
        staging[0] = total[3].astype(jnp.bfloat16)
        send_term(0, 0, term_sems.at[layer, 0], net.first)
        ffn_tile(layer, part, 1)
        staging[1] = total[1].astype(jnp.bfloat16)
        send_term(1, 1, term_sems.at[layer, 1], net.first)
        ffn_tile(layer, part, 2)
        net.arrival(landing.at[0], term_sems.at[layer, 0])
        staging[2] = (total[2] + landing[0].astype(jnp.float32)).astype(jnp.bfloat16)
        send_term(2, 2, term_sems.at[layer, 2], net.second)
        ffn_tile(layer, part, 0)
        pump(2)
        net.arrival(landing.at[1], term_sems.at[layer, 1])
        pump(1)
        net.arrival(landing.at[2], term_sems.at[layer, 2])

        def add(index, carry, last_layer=last_layer):
            span = pl.ds(pl.multiple_of(index * chunk, chunk), chunk)
            summed = stream[span, :] + (
                total[0, span, :]
                + landing[1, span, :].astype(jnp.float32)
                + landing[2, span, :].astype(jnp.float32)
            )
            if last_layer:
                out_ref[span, :] = summed.astype(out_ref.dtype)
            else:
                stream[span, :] = summed
            return carry

        lax.fori_loop(0, rows // chunk, add, 0)
        for sent in terms_sent:
            sent.wait_send()

    for condition, one in net.finish:
        guarded(condition, one.wait_send)


def head_window(head_size):
    reach = head_size + LANES - math.gcd(head_size, LANES)
    return -(-reach // LANES) * LANES


def fused_blocks(tokens, cond, norm_attn, norm_ffn, shards, chips_z):
    layers, share, width = shards[0].shape
    inner = shards[4].shape[2]
    tile = 256 if width % 256 == 0 else LANES
    tile_count = width // tile
    rows = tokens.shape[0]
    head_size = D // HEADS
    stages = layers * (1 + tile_count)
    sends = 1024
    shape = (layers, chips_z, width, tile, tile_count, head_size)
    anywhere = pl.BlockSpec(memory_space=pl.ANY)
    inside = pl.BlockSpec(memory_space=pltpu.VMEM)
    kind = tokens.dtype
    return pl.pallas_call(
        functools.partial(fused_kernel, shape),
        out_shape=jax.ShapeDtypeStruct((rows, width), kind),
        in_specs=[inside] * 4 + [anywhere] * 7,
        out_specs=inside,
        scratch_shapes=[
            pltpu.VMEM((layers, 7, PLANE, 2 * chips_z, share, width), kind),
            pltpu.VMEM((PLANE, rows, width), kind),
            pltpu.VMEM((3, rows, width), kind),
            pltpu.VMEM((3, rows, width), kind),
            pltpu.VMEM((PLANE, rows, width), jnp.float32),
            pltpu.VMEM((rows, width), jnp.float32),
            pltpu.SemaphoreType.DMA((layers * 7,)),
            pltpu.SemaphoreType.DMA((sends,)),
            pltpu.SemaphoreType.DMA((stages, chips_z)),
            pltpu.SemaphoreType.DMA((layers, PLANE, chips_z)),
            pltpu.SemaphoreType.DMA((layers, PLANE)),
            pltpu.SemaphoreType.DMA((layers, PLANE, chips_z)),
            pltpu.SemaphoreType.DMA((layers * tile_count, chips_z)),
            pltpu.SemaphoreType.DMA((layers, 3)),
            pltpu.SemaphoreType.DMA((layers, 3)),
        ],
        compiler_params=pltpu.CompilerParams(
            collective_id=0, has_side_effects=True, vmem_limit_bytes=67_000_000
        ),
        name="fused_blocks",
    )(tokens, cond, norm_attn, norm_ffn, *shards)


def attend(packed, head_size):
    total_rows = packed.shape[0]
    width = packed.shape[1] // 3
    set_rows = VIEWS * HW
    query_rows, sources = packed[:, :width], packed[:, width:]
    if total_rows % set_rows != 0:
        first = lax.axis_index("tp") * total_rows // set_rows * set_rows
        sources = lax.all_gather(sources, "tp", axis=0, tiled=True)
        sources = lax.dynamic_slice_in_dim(sources, first, set_rows, 0)
    set_count = sources.shape[0] // set_rows
    query_rows = query_rows.reshape(set_count, -1, width // head_size, head_size)
    key_rows = sources[:, :width].reshape(set_count, set_rows, -1, head_size)
    value_rows = sources[:, width:].reshape(set_count, set_rows, -1, head_size)
    scores = jnp.einsum(
        "bqhd,bkhd->bhqk", query_rows, key_rows, preferred_element_type=jnp.float32
    ) * head_size ** (-0.5)
    peak = jnp.max(scores, axis=-1, keepdims=True)
    expons = jnp.exp(scores - peak)
    attn_probs = (expons / jnp.sum(expons, axis=-1, keepdims=True)).astype(jnp.bfloat16)
    mixed_rows = jnp.einsum(
        "bhqk,bkhd->bqhd", attn_probs, value_rows, preferred_element_type=jnp.float32
    )
    return mixed_rows.astype(jnp.bfloat16).reshape(total_rows, width)


def out_terms(mixed_rows, weight):
    return lax.dot_general(
        mixed_rows, weight, (((1,), (1,)), ((), ())), preferred_element_type=jnp.float32
    )


def set_conditioning(view_ids, time_ids, camera_table):
    pose_range = jnp.arange(camera_table.shape[0], dtype=jnp.int32)
    onehot_pose = (view_ids[0][:, None] == pose_range[None, :]).astype(jnp.float32)
    camera = jnp.dot(onehot_pose, camera_table, precision=lax.Precision.HIGHEST)
    return camera + time_code(time_ids, camera_table.shape[1])


def body(
    tokens,
    view_ids,
    time_ids,
    camera_table,
    norm_attn,
    norm_ffn,
    w_query,
    w_key,
    w_value,
    w_out,
    w_gate,
    w_up,
    w_down,
):
    tp_count = lax.axis_size("tp")
    rep_count = lax.axis_size("rep")
    width = w_query.shape[2]
    inner = w_gate.shape[2]
    head_size = D // HEADS
    shards = (w_query, w_key, w_value, w_out, w_gate, w_up, w_down)
    share_rows = tokens.shape[0]
    fits = (
        rep_count == 2 * PLANE
        and share_rows == VIEWS * HW
        and time_ids.shape[0] == tp_count
        and inner == PLANE * width
        and w_query.shape[1] % 8 == 0
    )
    if fits:
        here = lax.axis_index("tp")
        cond = set_conditioning(
            lax.dynamic_slice_in_dim(view_ids, here, 1, 0),
            lax.dynamic_slice_in_dim(time_ids, here, 1, 0),
            camera_table,
        )
        return fused_blocks(tokens, cond, norm_attn, norm_ffn, shards, tp_count)

    row_ids = lax.axis_index("tp") * share_rows + jnp.arange(share_rows, dtype=jnp.int32)
    stream = tokens.astype(jnp.float32) + conditioning(row_ids, view_ids, time_ids, camera_table)

    def whole_weight(layer_index, first, count, after):
        own = [shard[layer_index] for shard in shards[first : first + count]]
        own, _ = lax.optimization_barrier((own, after))
        return lax.all_gather(jnp.concatenate(own, axis=1), ("rep", "tp"), axis=0, tiled=True)

    for layer_index in range(LAYERS):
        normed = layer_norm(stream, norm_attn[layer_index])
        qkv_w = whole_weight(layer_index, 0, 3, normed)
        packed = jnp.dot(normed, qkv_w, preferred_element_type=jnp.float32).astype(jnp.bfloat16)
        mixed_rows = attend(packed, head_size)
        stream = stream + out_terms(mixed_rows, whole_weight(layer_index, 3, 1, mixed_rows))
        normed = layer_norm(stream, norm_ffn[layer_index])
        gate_w = whole_weight(layer_index, 4, 1, normed)
        gate_part = jnp.dot(normed, gate_w, preferred_element_type=jnp.float32)
        up_w = whole_weight(layer_index, 5, 1, gate_part)
        up_part = jnp.dot(normed, up_w, preferred_element_type=jnp.float32)
        hidden = (jax.nn.gelu(gate_part, approximate=False) * up_part).astype(jnp.bfloat16)
        stream = stream + out_terms(hidden, whole_weight(layer_index, 6, 1, hidden))
    return stream.astype(jnp.bfloat16)


def solution(mesh):
    return jax.shard_map(
        body,
        mesh=mesh,
        in_specs=(
            P(("rep", "tp"), None),
            P("rep", None),
            P("rep"),
            P(),
            P(),
            P(),
            P(None, ("rep", "tp"), None),
            P(None, ("rep", "tp"), None),
            P(None, ("rep", "tp"), None),
            P(None, ("rep", "tp"), None),
            P(None, ("rep", "tp"), None),
            P(None, ("rep", "tp"), None),
            P(None, ("rep", "tp"), None),
        ),
        out_specs=P(("rep", "tp"), None),
        check_vma=False,
    )
```

```python
import functools
import math

import jax
import jax.numpy as jnp
from jax import lax
from jax.experimental import pallas as pl
from jax.experimental.pallas import tpu as pltpu
from jax.sharding import PartitionSpec as P

D = 1280
HEADS = 8
VIEWS = 4
HW = 64
LAYERS = 2


def layer_norm(activations, gain_vector):
    average = jnp.mean(activations, axis=-1, keepdims=True)
    centred = activations - average
    spread = jnp.mean(centred * centred, axis=-1, keepdims=True)
    return (centred * lax.rsqrt(spread + 1e-05) * gain_vector).astype(jnp.bfloat16)


def time_code(step_ids, width):
    half_width = width // 2
    frequency = jnp.exp(-math.log(10000.0) * jnp.arange(half_width, dtype=jnp.float32) / half_width)
    angles = step_ids.astype(jnp.float32)[:, None] * frequency[None, :]
    return jnp.concatenate([jnp.cos(angles), jnp.sin(angles)], axis=1)


def conditioning(row_ids, view_ids, time_ids, camera_table):
    set_ids = row_ids // (VIEWS * HW)
    slot_ids = set_ids * VIEWS + row_ids // HW % VIEWS
    flat_views = view_ids.reshape(-1)
    slot_range = jnp.arange(flat_views.shape[0], dtype=jnp.int32)
    pose_ids = jnp.sum(
        jnp.where(slot_ids[:, None] == slot_range[None, :], flat_views[None, :], 0), axis=1
    )
    set_range = jnp.arange(time_ids.shape[0], dtype=jnp.int32)
    step_ids = jnp.sum(
        jnp.where(set_ids[:, None] == set_range[None, :], time_ids[None, :], 0), axis=1
    )
    pose_range = jnp.arange(camera_table.shape[0], dtype=jnp.int32)
    onehot_pose = (pose_ids[:, None] == pose_range[None, :]).astype(jnp.float32)
    camera = jnp.dot(onehot_pose, camera_table, precision=lax.Precision.HIGHEST)
    return camera + time_code(step_ids, camera_table.shape[1])


MESH = pl.DeviceIdType.MESH
LANES = 128
ATTN, FFN = range(2)
(
    LINE,
    OUT,
    NEAR,
    FAR,
    COLUMNS,
    PAIRS_ATTN,
    PAIRS_FFN,
    EMBED,
    NORM,
    PROJECT,
    MIX,
    PROJECT_OUT,
    ROWS_OUT,
    ROWS_ON,
    ROWS_IN,
    ROWS_DONE,
    TILES,
    TERM,
    TERM_IN,
    RESIDUAL,
) = range(20)
PLANE = 4
POOL = 96
NAMED = 12
PARTS = ((0, 3), (3, 4))
SLOTS = (0, 2, 1, 3)


class Pieces:
    def __init__(self, chips_z, layers, tile_count, send_sems):
        self.chips_z, self.layers, self.tile_count = chips_z, layers, tile_count
        self.send_sems = send_sems
        self.used = 0
        self.named = 0
        self.finish = []
        rep_here = lax.axis_index("rep")
        self.z = lax.axis_index("tp")
        self.q = rep_here // 2
        self.core = rep_here % 2
        flip_x = self.q + 1 - 2 * (self.q % 2)
        flip_y = (self.q + 2) % PLANE
        self.first = flip_x + self.core * (flip_y - flip_x)
        self.second = flip_y + self.core * (flip_x - flip_y)
        self.diagonal = PLANE - 1 - self.q

    def at(self, q, core, z):
        return (q * 2 + core, z)

    def sibling(self):
        return self.at(self.q, 1 - self.core, self.z)

    def peer(self, q):
        return self.at(q, self.core, self.z)

    def line(self, step):
        return self.at(self.q, self.core, self.z + step)

    def copy(self, source, target, arrived, device, condition=None, later=True):
        if later:
            if len(self.finish) == POOL:
                guarded(*self.finish.pop(0))
            place = self.used % POOL
            self.used += 1
        else:
            place = POOL + self.named % NAMED
            self.named += 1
        one = pltpu.make_async_remote_copy(
            src_ref=source,
            dst_ref=target,
            send_sem=self.send_sems.at[place],
            recv_sem=arrived,
            device_id=device,
            device_id_type=MESH,
        )
        if later:
            self.finish.append((condition, one.wait_send))
        return one

    def arrival(self, region, arrived):
        pltpu.make_async_remote_copy(
            src_ref=region,
            dst_ref=region,
            send_sem=self.send_sems.at[0],
            recv_sem=arrived,
            device_id=self.sibling(),
            device_id_type=MESH,
        ).wait_recv()


def both(first, second):
    if first is None or second is None:
        return second if first is None else first
    return jnp.logical_and(first, second)


def guarded(condition, action):
    if condition is None:
        action()
    else:
        pl.when(condition)(action)


def fused_kernel(
    shape,
    tokens_ref,
    view_ids_ref,
    time_ids_ref,
    table_ref,
    gain_attn_ref,
    gain_ffn_ref,
    wq_ref,
    wk_ref,
    wv_ref,
    wo_ref,
    wg_ref,
    wu_ref,
    wd_ref,
    out_ref,
    full,
    normed,
    landing,
    staging,
    total,
    stream,
    own_sems,
    send_sems,
    line_sems,
    plane_sems,
    share_sems,
    pair_attn_sems,
    pair_ffn_sems,
    rows_sems,
    term_sems,
):
    layers, chips_z, width, tile, tile_count, head_size = shape
    net = Pieces(chips_z, layers, tile_count, send_sems)
    z, q, core = net.z, net.q, net.core
    rows = stream.shape[0]
    here = core * chips_z + z

    def attn_piece(layer, part, q_from, core_from, z_from):
        first_kind, last_kind = PARTS[part]
        return full.at[
            layer, first_kind:last_kind, q_from, core_from * chips_z + z_from
        ]

    def ffn_piece(layer, part, core_from, z_from):
        return full.at[
            layer, 4:7, :, core_from * chips_z + z_from, :, pl.ds(part * tile, tile)
        ]

    def in_line(offset):
        if offset == 0:
            return None
        return z + offset < chips_z if offset > 0 else z + offset >= 0

    def beyond(step):
        return z < chips_z - 1 if step > 0 else z > 0

    own = []
    for layer in range(layers):
        for first_kind, last_kind in PARTS:
            group = []
            for kind in range(first_kind, last_kind):
                ref = (wq_ref, wk_ref, wv_ref, wo_ref)[kind]
                group.append((ref.at[layer], full.at[layer, kind, q, here]))
            own.append(group)
    for layer in range(layers):
        group = []
        for kind, ref in enumerate((wg_ref, wu_ref, wd_ref)):
            group.append(
                (ref.at[layer, :, pl.ds(q * width, width)], full.at[layer, 4 + kind, q, here])
            )
        own.append(group)
    local, slot = [], 0
    for group in own:
        copies = []
        for source, target in group:
            copies.append(pltpu.make_async_copy(source, target, own_sems.at[slot]))
            copies[-1].start()
            slot += 1
        local.append(copies)

    def wait_local(index):
        for one in local[index]:
            one.wait()

    barrier = pltpu.get_barrier_semaphore()
    for device in (
        net.sibling(),
        net.peer(net.first),
        net.peer(net.second),
        net.peer(net.diagonal),
    ):
        pl.semaphore_signal(barrier, inc=1, device_id=device, device_id_type=MESH)
    for step in (1, -1):
        def greet(step=step):
            pl.semaphore_signal(barrier, inc=1, device_id=net.line(step), device_id_type=MESH)
        pl.when(beyond(step))(greet)
    count = jnp.int32(4) + (z > 0).astype(jnp.int32) + (z < chips_z - 1).astype(jnp.int32)
    pl.semaphore_wait(barrier, count)

    def along_line(stage, region, pair_sem, offset):
        z_from = z + offset
        valid = in_line(offset)
        sends = []
        for step in (1, -1):
            if offset == 0 or (offset > 0) == (step < 0):
                ahead = beyond(step)
                one = net.copy(
                    region,
                    region,
                    line_sems.at[stage, z_from],
                    net.line(step),
                    both(valid, ahead),
                )
                sends.append((ahead, one))
        share = net.copy(region, region, pair_sem, net.sibling(), valid)

        def action():
            if offset:
                net.arrival(region, line_sems.at[stage, z_from])
            for ahead, one in sends:
                guarded(ahead, one.start)
            share.start()

        guarded(valid, action)

    def attn_line(layer, part, offset):
        stage = layer * len(PARTS) + part
        along_line(
            stage,
            attn_piece(layer, part, q, core, z + offset),
            pair_attn_sems.at[stage],
            offset,
        )

    def attn_plane(layer, part, offset):
        stage = layer * len(PARTS) + part
        z_from = z + offset
        valid = in_line(offset)
        region = attn_piece(layer, part, q, core, z_from)
        sends = [
            net.copy(region, region, plane_sems.at[stage, q, z_from], net.peer(peer), valid)
            for peer in (net.first, net.second)
        ]

        def action():
            for one in sends:
                one.start()

        guarded(valid, action)

    def from_plane(layer, part, offset, which):
        stage = layer * len(PARTS) + part
        z_from = z + offset
        valid = in_line(offset)
        peer = (net.first, net.second, net.diagonal)[which]
        region = attn_piece(layer, part, peer, core, z_from)
        arrived = plane_sems.at[stage, peer, z_from]
        sends = []
        if which == 0:
            sends.append(net.copy(region, region, arrived, net.peer(net.second), valid))
        sends.append(
            net.copy(region, region, pair_attn_sems.at[stage], net.sibling(), valid)
        )

        def action():
            net.arrival(region, arrived)
            for one in sends:
                one.start()

        guarded(valid, action)

    def attn_pairs(layer, part):
        first_kind, last_kind = PARTS[part]
        net.arrival(
            full.at[layer, first_kind:last_kind, :, pl.ds((1 - core) * chips_z, chips_z)],
            pair_attn_sems.at[layer * len(PARTS) + part],
        )

    def exchange_columns(layer):
        for peer in (net.first, net.second, net.diagonal):
            for kind, ref in enumerate((wg_ref, wu_ref, wd_ref)):
                net.copy(
                    ref.at[layer, :, pl.ds(peer * width, width)],
                    full.at[layer, 4 + kind, q, here],
                    share_sems.at[layer, q],
                    net.peer(peer),
                ).start()

    def columns_here(layer):
        wait_local(layers * len(PARTS) + layer)
        for peer in (net.first, net.second, net.diagonal):
            net.arrival(full.at[layer, 4:7, peer, here], share_sems.at[layer, peer])

    def ffn_line(layer, part, offset):
        along_line(
            layers * len(PARTS) + layer * tile_count + part,
            ffn_piece(layer, part, core, z + offset),
            pair_ffn_sems.at[layer * tile_count + part],
            offset,
        )

    def ffn_pairs(layer, part):
        span = pl.ds(part * tile, tile)
        net.arrival(
            full.at[layer, 4:7, :, pl.ds((1 - core) * chips_z, chips_z), :, span],
            pair_ffn_sems.at[layer * tile_count + part],
        )

    def offsets(hops):
        return [hops, -hops] if hops else [0]

    def offsets(hops):
        return [hops, -hops] if hops else [0]

    chunk = 64 if rows % 64 == 0 else rows

    def embed():
        views = view_ids_ref.shape[1]
        per_view = rows // views
        half_width = width // 2
        place = lax.broadcasted_iota(jnp.int32, (1, half_width), 1).astype(jnp.float32)
        frequency = jnp.exp(-math.log(10000.0) * place / half_width)
        angles = time_ids_ref[z].astype(jnp.float32) * frequency
        code = jnp.concatenate([jnp.cos(angles), jnp.sin(angles)], axis=1)
        pose = lax.broadcasted_iota(jnp.int32, (table_ref.shape[0], 1), 0)
        for view in range(views):
            span = pl.ds(view * per_view, per_view)
            camera = jnp.sum(
                jnp.where(pose == view_ids_ref[z, view], table_ref[...], 0.0),
                axis=0,
                keepdims=True,
            )
            stream[span, :] = tokens_ref[span, :].astype(jnp.float32) + (camera + code)

    def normalise(gain_ref, layer):
        def one(index, carry):
            span = pl.ds(pl.multiple_of(index * chunk, chunk), chunk)
            normed[0, span, :] = layer_norm(stream[span, :], gain_ref[layer : layer + 1, :])
            return carry

        lax.fori_loop(0, rows // chunk, one, 0)

    def weight(layer, kind, index, size):
        span = pl.ds(pl.multiple_of(index * size, size), size)
        return full[layer, kind, :, :, :, span].reshape(width, size)

    column = 256 if width % 256 == 0 else LANES

    def project(layer, kind):
        def one(index, carry):
            span = pl.ds(pl.multiple_of(index * column, column), column)
            staging[kind, :, span] = jnp.dot(
                normed[0], weight(layer, kind, index, column), preferred_element_type=jnp.float32
            ).astype(jnp.bfloat16)
            return carry

        lax.fori_loop(0, width // column, one, 0)

    window = head_window(head_size)

    def attend_heads(first_head, last_head):
        def one(head, carry):
            start = head * head_size
            base = pl.multiple_of(start // LANES * LANES, LANES)
            span = pl.ds(base, window)
            lane = lax.broadcasted_iota(jnp.int32, (1, window), 1) + base
            inside = jnp.logical_and(lane >= start, lane < start + head_size)
            query = staging[0, :, span]
            scores = out_terms(
                jnp.where(inside, query, jnp.zeros_like(query)), staging[1, :, span]
            ) * head_size ** (-0.5)
            peak = jnp.max(scores, axis=-1, keepdims=True)
            expons = jnp.exp(scores - peak)
            probs = (expons / jnp.sum(expons, axis=-1, keepdims=True)).astype(jnp.bfloat16)
            mixed = jnp.dot(
                probs, staging[2, :, span], preferred_element_type=jnp.float32
            ).astype(jnp.bfloat16)
            staging[0, :, span] = jnp.where(inside, mixed, query)
            return carry

        lax.fori_loop(first_head, last_head, one, 0)

    def project_out(layer):
        def one(index, carry):
            span = pl.ds(pl.multiple_of(index * column, column), column)
            stream[...] += out_terms(staging[0, :, span], weight(layer, 3, index, column))
            return carry

        lax.fori_loop(0, width // column, one, 0)

    half = rows // 2

    def ffn_tile(layer, part, unit):
        pair = pl.ds(unit % 2 * 2, 2)
        span = pl.ds(pl.multiple_of(unit // 2 * half, half), half)
        acts = normed[pair, span, :].reshape(2 * half, width)
        gate = jnp.dot(acts, weight(layer, 4, part, tile), preferred_element_type=jnp.float32)
        up = jnp.dot(acts, weight(layer, 5, part, tile), preferred_element_type=jnp.float32)
        gate = 0.5 * gate * (1.0 + lax.erf(gate * math.sqrt(0.5)))
        hidden = (gate * up).astype(jnp.bfloat16)
        term = out_terms(hidden, weight(layer, 6, part, tile)).reshape(2, half, width)
        if part == 0:
            total[pair, span, :] = term
        else:
            total[pair, span, :] = total[pair, span, :] + term

    def head_of(part):
        count = D // head_size
        return count * part // 2

    rows_sent, terms_sent = [], []

    def half_span(index):
        return pl.ds(index * half, half)

    def send_rows(layer, index, role, target, side):
        span = half_span(index)
        rows_sent.append(
            net.copy(
                normed.at[SLOTS[role], span],
                normed.at[SLOTS[target], span],
                rows_sems.at[layer, index, target - 1],
                net.peer((net.first, net.second)[side]),
                later=False,
            )
        )
        rows_sent[-1].start()

    def rows_arrival(layer, index, role):
        net.arrival(
            normed.at[SLOTS[role], half_span(index)], rows_sems.at[layer, index, role - 1]
        )

    def term_arrival(layer, index, target):
        net.arrival(
            landing.at[target, half_span(index)], term_sems.at[layer, index, target]
        )

    def send_term(layer, index, target):
        span = half_span(index)
        role = (3, 1, 2)[target]
        value = total[SLOTS[role], span, :]
        if target == 2:
            term_arrival(layer, index, 0)
            value = value + landing[0, span, :].astype(jnp.float32)
        staging[target, span, :] = value.astype(jnp.bfloat16)
        terms_sent.append(
            net.copy(
                staging.at[target, span],
                landing.at[target, span],
                term_sems.at[layer, index, target],
                net.peer((net.first, net.first, net.second)[target]),
                later=False,
            )
        )
        terms_sent[-1].start()

    def settle(copies):
        for one in copies:
            one.wait_send()
        copies.clear()

    def residual(layer):
        last_layer = layer == layers - 1

        def add(index, carry):
            span = pl.ds(pl.multiple_of(index * chunk, chunk), chunk)
            summed = stream[span, :] + (
                total[SLOTS[0], span, :]
                + landing[1, span, :].astype(jnp.float32)
                + landing[2, span, :].astype(jnp.float32)
            )
            if last_layer:
                out_ref[span, :] = summed.astype(out_ref.dtype)
            else:
                stream[span, :] = summed
            return carry

        lax.fori_loop(0, rows // chunk, add, 0)
        settle(terms_sent)

    def piece(kind, layer, part, hops):
        if kind == ATTN:
            if hops == 0:
                wait_local(layer * len(PARTS) + part)
            for offset in offsets(hops):
                attn_line(layer, part, offset)
        else:
            if hops == 0 and part == 0:
                columns_here(layer)
            for offset in offsets(hops):
                ffn_line(layer, part, offset)

    def tiles(layer, part, first_unit, last_unit):
        if last_unit - first_unit == 1:
            ffn_tile(layer, part, first_unit)
            return

        def one(unit, carry):
            ffn_tile(layer, part, unit)
            return carry

        lax.fori_loop(first_unit, last_unit, one, 0)

    def run(token):
        name, rest = token[0], token[1:]
        if name == LINE:
            piece(*rest)
        elif name == OUT:
            for offset in offsets(rest[2]):
                attn_plane(rest[0], rest[1], offset)
        elif name == NEAR:
            for offset in offsets(rest[2]):
                from_plane(rest[0], rest[1], offset, 0)
                from_plane(rest[0], rest[1], offset, 1)
        elif name == FAR:
            for offset in offsets(rest[2]):
                from_plane(rest[0], rest[1], offset, 2)
        elif name == COLUMNS:
            exchange_columns(rest[0])
        elif name == PAIRS_ATTN:
            attn_pairs(*rest)
        elif name == PAIRS_FFN:
            ffn_pairs(*rest)
        elif name == EMBED:
            embed()
        elif name == NORM:
            normalise((gain_attn_ref, gain_ffn_ref)[rest[1]], rest[0])
        elif name == PROJECT:
            project(*rest)
        elif name == MIX:
            attend_heads(head_of(rest[1]), head_of(rest[1] + 1))
        elif name == PROJECT_OUT:
            project_out(rest[0])
        elif name == ROWS_OUT:
            send_rows(rest[0], rest[1], 0, 1, 0)
            send_rows(rest[0], rest[1], 0, 2, 1)
        elif name == ROWS_ON:
            rows_arrival(rest[0], rest[1], 1)
            send_rows(rest[0], rest[1], 1, 3, 1)
        elif name == ROWS_IN:
            rows_arrival(*rest)
        elif name == ROWS_DONE:
            settle(rows_sent)
        elif name == TILES:
            tiles(*rest)
        elif name == TERM:
            send_term(*rest)
        elif name == TERM_IN:
            term_arrival(*rest)
        elif name == RESIDUAL:
            residual(rest[0])

    for token in schedule(chips_z, layers, tile_count):
        run(token)
    for condition, action in net.finish:
        guarded(condition, action)


def merged(tokens):
    out = []
    for token in tokens:
        if token[0] == TILES:
            layer, part, index, first_pair, count = token[1:]
            first = 2 * index + first_pair
            token = (TILES, layer, part, first, first + count)
            previous = out[-1]
            if previous[:3] == token[:3] and previous[4] == first:
                out[-1] = previous[:4] + (first + count,)
                continue
        out.append(token)
    return out


def schedule(chips_z, layers, tile_count):
    if (chips_z, layers, tile_count) == (4, 2, 5):
        return merged(ORDER)
    return merged(plain_schedule(chips_z, layers, tile_count))


def plain_schedule(chips_z, layers, tile_count):
    tokens = [(COLUMNS, 0), (EMBED,), (NORM, 0, 0)]
    for layer in range(layers):
        if layer:
            tokens.append((COLUMNS, layer))
        for part in range(len(PARTS)):
            for hops in range(chips_z):
                tokens += [(LINE, ATTN, layer, part, hops), (OUT, layer, part, hops)]
                tokens += [(NEAR, layer, part, hops), (FAR, layer, part, hops)]
            tokens.append((PAIRS_ATTN, layer, part))
        if layer:
            tokens.append((NORM, layer, 0))
        tokens += [(PROJECT, layer, kind) for kind in range(3)]
        tokens += [(MIX, layer, 0), (MIX, layer, 1), (PROJECT_OUT, layer)]
        tokens.append((NORM, layer, 1))
        tokens += [(ROWS_OUT, layer, 0), (ROWS_OUT, layer, 1)]
        for index in range(2):
            tokens += [(ROWS_ON, layer, index), (ROWS_IN, layer, index, 2)]
            tokens.append((ROWS_IN, layer, index, 3))
        for part in range(tile_count):
            tokens += [(LINE, FFN, layer, part, hops) for hops in range(chips_z)]
            tokens.append((PAIRS_FFN, layer, part))
            tokens += [(TILES, layer, part, index, 0, 2) for index in range(2)]
        tokens.append((ROWS_DONE, layer))
        for target in range(3):
            tokens += [(TERM, layer, index, target) for index in range(2)]
        for target in (1, 2):
            tokens += [(TERM_IN, layer, index, target) for index in range(2)]
        tokens.append((RESIDUAL, layer))
    return tokens


ORDER = (
    (LINE, ATTN, 0, 0, 0), (LINE, ATTN, 1, 0, 0), (LINE, ATTN, 0, 1, 0), (OUT, 0, 1, 0),
    (COLUMNS, 0), (LINE, ATTN, 0, 0, 1), (OUT, 0, 0, 0), (LINE, ATTN, 1, 1, 0),
    (LINE, ATTN, 0, 1, 1), (OUT, 0, 0, 1), (LINE, ATTN, 1, 0, 1), (LINE, ATTN, 0, 0, 2),
    (OUT, 0, 0, 2), (OUT, 0, 1, 1), (LINE, ATTN, 0, 1, 2), (EMBED,), (NEAR, 0, 0, 1),
    (OUT, 0, 1, 2), (LINE, ATTN, 1, 1, 1), (LINE, FFN, 0, 0, 0), (OUT, 1, 0, 0),
    (LINE, ATTN, 0, 0, 3), (LINE, FFN, 0, 1, 0), (LINE, ATTN, 0, 1, 3), (OUT, 0, 0, 3),
    (LINE, ATTN, 1, 0, 2), (NEAR, 0, 1, 2), (LINE, FFN, 0, 0, 1), (NEAR, 0, 0, 3),
    (OUT, 0, 1, 3), (NEAR, 0, 0, 0), (NEAR, 0, 0, 2), (LINE, FFN, 0, 1, 1), (LINE, FFN, 0, 0, 2),
    (NEAR, 0, 1, 0), (FAR, 0, 0, 0), (NEAR, 0, 1, 1), (NEAR, 0, 1, 3), (NEAR, 1, 0, 0),
    (NORM, 0, 0), (FAR, 0, 0, 1), (COLUMNS, 1), (OUT, 1, 1, 0), (LINE, FFN, 0, 4, 0),
    (OUT, 1, 0, 1), (FAR, 0, 1, 0), (LINE, ATTN, 1, 1, 2), (FAR, 0, 1, 2), (LINE, FFN, 0, 2, 0),
    (FAR, 0, 0, 3), (FAR, 0, 0, 2), (PAIRS_ATTN, 0, 0), (LINE, ATTN, 1, 0, 3), (PROJECT, 0, 0),
    (PROJECT, 0, 1), (FAR, 0, 1, 3), (PROJECT, 0, 2), (FAR, 0, 1, 1), (MIX, 0, 0), (MIX, 0, 1),
    (PAIRS_ATTN, 0, 1), (LINE, FFN, 0, 4, 1), (OUT, 1, 0, 3), (LINE, FFN, 0, 3, 0),
    (PROJECT_OUT, 0), (NORM, 0, 1), (LINE, FFN, 0, 2, 1), (LINE, FFN, 0, 0, 3),
    (LINE, FFN, 0, 4, 2), (ROWS_OUT, 0, 0), (PAIRS_FFN, 0, 0), (LINE, FFN, 0, 3, 1),
    (LINE, ATTN, 1, 1, 3), (ROWS_OUT, 0, 1), (LINE, FFN, 0, 2, 2), (ROWS_ON, 0, 1),
    (LINE, FFN, 0, 1, 2), (ROWS_ON, 0, 0), (ROWS_IN, 0, 1, 3), (LINE, FFN, 0, 2, 3),
    (NEAR, 1, 0, 3), (LINE, FFN, 0, 1, 3), (ROWS_IN, 0, 1, 2), (OUT, 1, 0, 2),
    (LINE, FFN, 0, 3, 2), (LINE, FFN, 1, 0, 0), (TILES, 0, 0, 1, 0, 2), (PAIRS_FFN, 0, 2),
    (ROWS_IN, 0, 0, 3), (LINE, FFN, 0, 4, 3), (NEAR, 1, 0, 1), (LINE, FFN, 1, 1, 0),
    (ROWS_IN, 0, 0, 2), (PAIRS_FFN, 0, 1), (FAR, 1, 0, 0), (LINE, FFN, 1, 2, 0),
    (LINE, FFN, 1, 3, 0), (FAR, 1, 0, 3), (TILES, 0, 0, 0, 0, 2), (ROWS_DONE, 0),
    (LINE, FFN, 1, 4, 0), (OUT, 1, 1, 2), (TILES, 0, 1, 0, 0, 2), (PAIRS_FFN, 0, 4),
    (TILES, 0, 1, 1, 0, 2), (LINE, FFN, 0, 3, 3), (NEAR, 1, 0, 2), (TILES, 0, 2, 1, 0, 2),
    (PAIRS_FFN, 0, 3), (OUT, 1, 1, 3), (TILES, 0, 3, 1, 0, 2), (TILES, 0, 4, 1, 1, 1),
    (FAR, 1, 0, 1), (TERM, 0, 1, 1), (TERM, 0, 1, 0), (TILES, 0, 2, 0, 0, 2),
    (TILES, 0, 3, 0, 0, 2), (TILES, 0, 4, 0, 1, 1), (TILES, 0, 4, 1, 0, 1), (TERM, 0, 0, 0),
    (NEAR, 1, 1, 0), (NEAR, 1, 1, 3), (LINE, FFN, 1, 2, 1), (TILES, 0, 4, 0, 0, 1),
    (FAR, 1, 0, 2), (TERM, 0, 1, 2), (LINE, FFN, 1, 0, 1), (TERM, 0, 0, 2), (TERM, 0, 0, 1),
    (TERM_IN, 0, 1, 1), (LINE, FFN, 1, 1, 1), (OUT, 1, 1, 1), (TERM_IN, 0, 0, 2),
    (TERM_IN, 0, 0, 1), (TERM_IN, 0, 1, 2), (FAR, 1, 1, 3), (LINE, FFN, 1, 4, 1),
    (PAIRS_ATTN, 1, 0), (LINE, FFN, 1, 3, 1), (RESIDUAL, 0), (NORM, 1, 0), (NEAR, 1, 1, 2),
    (PROJECT, 1, 0), (NEAR, 1, 1, 1), (LINE, FFN, 1, 0, 2), (PROJECT, 1, 1), (FAR, 1, 1, 0),
    (FAR, 1, 1, 2), (LINE, FFN, 1, 2, 2), (PROJECT, 1, 2), (FAR, 1, 1, 1), (MIX, 1, 0),
    (MIX, 1, 1), (PAIRS_ATTN, 1, 1), (PROJECT_OUT, 1), (NORM, 1, 1), (ROWS_OUT, 1, 0),
    (LINE, FFN, 1, 1, 2), (LINE, FFN, 1, 3, 2), (LINE, FFN, 1, 2, 3), (ROWS_ON, 1, 0),
    (ROWS_OUT, 1, 1), (LINE, FFN, 1, 0, 3), (PAIRS_FFN, 1, 0), (ROWS_IN, 1, 0, 3),
    (LINE, FFN, 1, 1, 3), (LINE, FFN, 1, 4, 2), (PAIRS_FFN, 1, 2), (ROWS_IN, 1, 0, 2),
    (TILES, 1, 0, 0, 0, 2), (ROWS_ON, 1, 1), (LINE, FFN, 1, 3, 3), (PAIRS_FFN, 1, 1),
    (TILES, 1, 1, 0, 0, 2), (TILES, 1, 2, 0, 0, 2), (ROWS_IN, 1, 1, 2), (LINE, FFN, 1, 4, 3),
    (PAIRS_FFN, 1, 3), (TILES, 1, 3, 0, 0, 2), (PAIRS_FFN, 1, 4), (TILES, 1, 4, 0, 1, 1),
    (ROWS_IN, 1, 1, 3), (ROWS_DONE, 1), (TERM, 1, 0, 0), (TILES, 1, 0, 1, 0, 2),
    (TILES, 1, 4, 0, 0, 1), (TERM, 1, 0, 1), (TILES, 1, 1, 1, 0, 2), (TILES, 1, 2, 1, 0, 2),
    (TERM, 1, 0, 2), (TILES, 1, 3, 1, 0, 2), (TILES, 1, 4, 1, 1, 1), (TERM, 1, 1, 0),
    (TILES, 1, 4, 1, 0, 1), (TERM, 1, 1, 1), (TERM, 1, 1, 2), (TERM_IN, 1, 1, 2),
    (TERM_IN, 1, 0, 1), (TERM_IN, 1, 1, 1), (TERM_IN, 1, 0, 2), (RESIDUAL, 1),
)


def head_window(head_size):
    reach = head_size + LANES - math.gcd(head_size, LANES)
    return -(-reach // LANES) * LANES


def fused_blocks(tokens, view_ids, time_ids, camera_table, norm_attn, norm_ffn, shards, chips_z):
    layers, share, width = shards[0].shape
    inner = shards[4].shape[2]
    tile = 256 if width % 256 == 0 else LANES
    tile_count = width // tile
    rows = tokens.shape[0]
    head_size = D // HEADS
    stages = layers * (len(PARTS) + tile_count)
    shape = (layers, chips_z, width, tile, tile_count, head_size)
    anywhere = pl.BlockSpec(memory_space=pl.ANY)
    inside = pl.BlockSpec(memory_space=pltpu.VMEM)
    scalars = pl.BlockSpec(memory_space=pltpu.SMEM)
    kind = tokens.dtype
    return pl.pallas_call(
        functools.partial(fused_kernel, shape),
        out_shape=jax.ShapeDtypeStruct((rows, width), kind),
        in_specs=[inside, scalars, scalars] + [inside] * 3 + [anywhere] * 7,
        out_specs=inside,
        scratch_shapes=[
            pltpu.VMEM((layers, 7, PLANE, 2 * chips_z, share, width), kind),
            pltpu.VMEM((PLANE, rows, width), kind),
            pltpu.VMEM((3, rows, width), kind),
            pltpu.VMEM((3, rows, width), kind),
            pltpu.VMEM((PLANE, rows, width), jnp.float32),
            pltpu.VMEM((rows, width), jnp.float32),
            pltpu.SemaphoreType.DMA((layers * 7,)),
            pltpu.SemaphoreType.DMA((POOL + NAMED,)),
            pltpu.SemaphoreType.DMA((stages, chips_z)),
            pltpu.SemaphoreType.DMA((layers * len(PARTS), PLANE, chips_z)),
            pltpu.SemaphoreType.DMA((layers, PLANE)),
            pltpu.SemaphoreType.DMA((layers * len(PARTS),)),
            pltpu.SemaphoreType.DMA((layers * tile_count,)),
            pltpu.SemaphoreType.DMA((layers, 2, 3)),
            pltpu.SemaphoreType.DMA((layers, 2, 3)),
        ],
        compiler_params=pltpu.CompilerParams(
            collective_id=0, has_side_effects=True, vmem_limit_bytes=67_000_000
        ),
        name="fused_blocks",
    )(tokens, view_ids, time_ids, camera_table, norm_attn, norm_ffn, *shards)


def attend(packed, head_size):
    total_rows = packed.shape[0]
    width = packed.shape[1] // 3
    set_rows = VIEWS * HW
    query_rows, sources = packed[:, :width], packed[:, width:]
    if total_rows % set_rows != 0:
        first = lax.axis_index("tp") * total_rows // set_rows * set_rows
        sources = lax.all_gather(sources, "tp", axis=0, tiled=True)
        sources = lax.dynamic_slice_in_dim(sources, first, set_rows, 0)
    set_count = sources.shape[0] // set_rows
    query_rows = query_rows.reshape(set_count, -1, width // head_size, head_size)
    key_rows = sources[:, :width].reshape(set_count, set_rows, -1, head_size)
    value_rows = sources[:, width:].reshape(set_count, set_rows, -1, head_size)
    scores = jnp.einsum(
        "bqhd,bkhd->bhqk", query_rows, key_rows, preferred_element_type=jnp.float32
    ) * head_size ** (-0.5)
    peak = jnp.max(scores, axis=-1, keepdims=True)
    expons = jnp.exp(scores - peak)
    attn_probs = (expons / jnp.sum(expons, axis=-1, keepdims=True)).astype(jnp.bfloat16)
    mixed_rows = jnp.einsum(
        "bhqk,bkhd->bqhd", attn_probs, value_rows, preferred_element_type=jnp.float32
    )
    return mixed_rows.astype(jnp.bfloat16).reshape(total_rows, width)


def out_terms(mixed_rows, weight):
    return lax.dot_general(
        mixed_rows, weight, (((1,), (1,)), ((), ())), preferred_element_type=jnp.float32
    )


def body(
    tokens,
    view_ids,
    time_ids,
    camera_table,
    norm_attn,
    norm_ffn,
    w_query,
    w_key,
    w_value,
    w_out,
    w_gate,
    w_up,
    w_down,
):
    tp_count = lax.axis_size("tp")
    rep_count = lax.axis_size("rep")
    width = w_query.shape[2]
    inner = w_gate.shape[2]
    head_size = D // HEADS
    shards = (w_query, w_key, w_value, w_out, w_gate, w_up, w_down)
    share_rows = tokens.shape[0]
    fits = (
        rep_count == 2 * PLANE
        and share_rows == VIEWS * HW
        and time_ids.shape[0] == tp_count
        and inner == PLANE * width
        and w_query.shape[1] % 8 == 0
        and share_rows % 32 == 0
    )
    if fits:
        return fused_blocks(
            tokens, view_ids, time_ids, camera_table, norm_attn, norm_ffn, shards, tp_count
        )

    row_ids = lax.axis_index("tp") * share_rows + jnp.arange(share_rows, dtype=jnp.int32)
    stream = tokens.astype(jnp.float32) + conditioning(row_ids, view_ids, time_ids, camera_table)

    def whole_weight(layer_index, first, count, after):
        own = [shard[layer_index] for shard in shards[first : first + count]]
        own, _ = lax.optimization_barrier((own, after))
        return lax.all_gather(jnp.concatenate(own, axis=1), ("rep", "tp"), axis=0, tiled=True)

    for layer_index in range(LAYERS):
        normed = layer_norm(stream, norm_attn[layer_index])
        qkv_w = whole_weight(layer_index, 0, 3, normed)
        packed = jnp.dot(normed, qkv_w, preferred_element_type=jnp.float32).astype(jnp.bfloat16)
        mixed_rows = attend(packed, head_size)
        stream = stream + out_terms(mixed_rows, whole_weight(layer_index, 3, 1, mixed_rows))
        normed = layer_norm(stream, norm_ffn[layer_index])
        gate_w = whole_weight(layer_index, 4, 1, normed)
        gate_part = jnp.dot(normed, gate_w, preferred_element_type=jnp.float32)
        up_w = whole_weight(layer_index, 5, 1, gate_part)
        up_part = jnp.dot(normed, up_w, preferred_element_type=jnp.float32)
        hidden = (jax.nn.gelu(gate_part, approximate=False) * up_part).astype(jnp.bfloat16)
        stream = stream + out_terms(hidden, whole_weight(layer_index, 6, 1, hidden))
    return stream.astype(jnp.bfloat16)


def solution(mesh):
    return jax.shard_map(
        body,
        mesh=mesh,
        in_specs=(
            P(("rep", "tp"), None),
            P("rep", None),
            P("rep"),
            P(),
            P(),
            P(),
            P(None, ("rep", "tp"), None),
            P(None, ("rep", "tp"), None),
            P(None, ("rep", "tp"), None),
            P(None, ("rep", "tp"), None),
            P(None, ("rep", "tp"), None),
            P(None, ("rep", "tp"), None),
            P(None, ("rep", "tp"), None),
        ),
        out_specs=P(("rep", "tp"), None),
        check_vma=False,
    )
```

```python
import functools
import math

import jax
import jax.numpy as jnp
from jax import lax
from jax.experimental import pallas as pl
from jax.experimental.pallas import tpu as pltpu
from jax.sharding import PartitionSpec as P

D = 1280
HEADS = 8
VIEWS = 4
HW = 64
LAYERS = 2


def layer_norm(activations, gain_vector):
    average = jnp.mean(activations, axis=-1, keepdims=True)
    centred = activations - average
    spread = jnp.mean(centred * centred, axis=-1, keepdims=True)
    return (centred * lax.rsqrt(spread + 1e-05) * gain_vector).astype(jnp.bfloat16)


def time_code(step_ids, width):
    half_width = width // 2
    frequency = jnp.exp(-math.log(10000.0) * jnp.arange(half_width, dtype=jnp.float32) / half_width)
    angles = step_ids.astype(jnp.float32)[:, None] * frequency[None, :]
    return jnp.concatenate([jnp.cos(angles), jnp.sin(angles)], axis=1)


def conditioning(row_ids, view_ids, time_ids, camera_table):
    set_ids = row_ids // (VIEWS * HW)
    slot_ids = set_ids * VIEWS + row_ids // HW % VIEWS
    flat_views = view_ids.reshape(-1)
    slot_range = jnp.arange(flat_views.shape[0], dtype=jnp.int32)
    pose_ids = jnp.sum(
        jnp.where(slot_ids[:, None] == slot_range[None, :], flat_views[None, :], 0), axis=1
    )
    set_range = jnp.arange(time_ids.shape[0], dtype=jnp.int32)
    step_ids = jnp.sum(
        jnp.where(set_ids[:, None] == set_range[None, :], time_ids[None, :], 0), axis=1
    )
    pose_range = jnp.arange(camera_table.shape[0], dtype=jnp.int32)
    onehot_pose = (pose_ids[:, None] == pose_range[None, :]).astype(jnp.float32)
    camera = jnp.dot(onehot_pose, camera_table, precision=lax.Precision.HIGHEST)
    return camera + time_code(step_ids, camera_table.shape[1])


MESH = pl.DeviceIdType.MESH
LANES = 128
ATTN, FFN = range(2)
(
    LINE,
    OUT,
    NEAR,
    FAR,
    COLUMNS,
    PAIRS_ATTN,
    PAIRS_FFN,
    EMBED,
    NORM,
    PROJECT,
    MIX,
    PROJECT_OUT,
    ROWS_OUT,
    ROWS_ON,
    ROWS_IN,
    ROWS_DONE,
    TILES,
    TERM,
    TERM_IN,
    RESIDUAL,
) = range(20)
PLANE = 4
POOL = 48
NAMED = 12
PARTS = ((0, 3), (3, 4))
SLOTS = (0, 2, 1, 3)


class Pieces:
    def __init__(self, chips_z, layers, tile_count, send_sems):
        self.chips_z, self.layers, self.tile_count = chips_z, layers, tile_count
        self.send_sems = send_sems
        self.used = 0
        self.named = 0
        self.finish = []
        rep_here = lax.axis_index("rep")
        self.z = lax.axis_index("tp")
        self.q = rep_here // 2
        self.core = rep_here % 2
        flip_x = self.q + 1 - 2 * (self.q % 2)
        flip_y = (self.q + 2) % PLANE
        self.first = flip_x + self.core * (flip_y - flip_x)
        self.second = flip_y + self.core * (flip_x - flip_y)
        self.diagonal = PLANE - 1 - self.q

    def at(self, q, core, z):
        return (q * 2 + core, z)

    def sibling(self):
        return self.at(self.q, 1 - self.core, self.z)

    def peer(self, q):
        return self.at(q, self.core, self.z)

    def line(self, step):
        return self.at(self.q, self.core, self.z + step)

    def copy(self, source, target, arrived, device, condition=None, later=True):
        if later:
            if len(self.finish) == POOL:
                guarded(*self.finish.pop(0))
            place = self.used % POOL
            self.used += 1
        else:
            place = POOL + self.named % NAMED
            self.named += 1
        one = pltpu.make_async_remote_copy(
            src_ref=source,
            dst_ref=target,
            send_sem=self.send_sems.at[place],
            recv_sem=arrived,
            device_id=device,
            device_id_type=MESH,
        )
        if later:
            self.finish.append((condition, one.wait_send))
        return one

    def arrival(self, region, arrived):
        pltpu.make_async_remote_copy(
            src_ref=region,
            dst_ref=region,
            send_sem=self.send_sems.at[0],
            recv_sem=arrived,
            device_id=self.sibling(),
            device_id_type=MESH,
        ).wait_recv()


def both(first, second):
    if first is None or second is None:
        return second if first is None else first
    return jnp.logical_and(first, second)


def guarded(condition, action):
    if condition is None:
        action()
    else:
        pl.when(condition)(action)


def fused_kernel(
    shape,
    tokens_ref,
    view_ids_ref,
    time_ids_ref,
    table_ref,
    gain_attn_ref,
    gain_ffn_ref,
    wq_ref,
    wk_ref,
    wv_ref,
    wo_ref,
    wg_ref,
    wu_ref,
    wd_ref,
    out_ref,
    full,
    normed,
    landing,
    staging,
    total,
    stream,
    tokens_in,
    table_in,
    own_sems,
    first_sems,
    send_sems,
    line_sems,
    plane_sems,
    share_sems,
    pair_attn_sems,
    pair_ffn_sems,
    rows_sems,
    term_sems,
):
    layers, chips_z, width, tile, tile_count, head_size = shape
    net = Pieces(chips_z, layers, tile_count, send_sems)
    z, q, core = net.z, net.q, net.core
    rows = stream.shape[0]
    here = core * chips_z + z

    def attn_piece(layer, part, q_from, core_from, z_from):
        first_kind, last_kind = PARTS[part]
        return full.at[
            layer, first_kind:last_kind, q_from, core_from * chips_z + z_from
        ]

    def ffn_piece(layer, part, core_from, z_from):
        return full.at[
            layer, 4:7, :, core_from * chips_z + z_from, :, pl.ds(part * tile, tile)
        ]

    def in_line(offset):
        if offset == 0:
            return None
        return z + offset < chips_z if offset > 0 else z + offset >= 0

    def beyond(step):
        return z < chips_z - 1 if step > 0 else z > 0

    own = []
    for layer in range(layers):
        for first_kind, last_kind in PARTS:
            group = []
            for kind in range(first_kind, last_kind):
                ref = (wq_ref, wk_ref, wv_ref, wo_ref)[kind]
                group.append((ref.at[layer], full.at[layer, kind, q, here]))
            own.append(group)
    for layer in range(layers):
        group = []
        for kind, ref in enumerate((wg_ref, wu_ref, wd_ref)):
            group.append(
                (ref.at[layer, :, pl.ds(q * width, width)], full.at[layer, 4 + kind, q, here])
            )
        own.append(group)
    local, slot = [], 0
    for group in own:
        copies = []
        for source, target in group:
            copies.append(pltpu.make_async_copy(source, target, own_sems.at[slot]))
            copies[-1].start()
            slot += 1
        local.append(copies)

    fetches = (
        pltpu.make_async_copy(tokens_ref, tokens_in, first_sems.at[0]),
        pltpu.make_async_copy(table_ref, table_in, first_sems.at[1]),
    )
    for one in fetches:
        one.start()

    def wait_local(index):
        for one in local[index]:
            one.wait()

    barrier = pltpu.get_barrier_semaphore()
    for device in (
        net.sibling(),
        net.peer(net.first),
        net.peer(net.second),
        net.peer(net.diagonal),
    ):
        pl.semaphore_signal(barrier, inc=1, device_id=device, device_id_type=MESH)
    for step in (1, -1):
        def greet(step=step):
            pl.semaphore_signal(barrier, inc=1, device_id=net.line(step), device_id_type=MESH)
        pl.when(beyond(step))(greet)
    count = jnp.int32(4) + (z > 0).astype(jnp.int32) + (z < chips_z - 1).astype(jnp.int32)
    pl.semaphore_wait(barrier, count)

    def along_line(stage, region, pair_sem, offset):
        z_from = z + offset
        valid = in_line(offset)
        sends = []
        for step in (1, -1):
            if offset == 0 or (offset > 0) == (step < 0):
                ahead = beyond(step)
                one = net.copy(
                    region,
                    region,
                    line_sems.at[stage, z_from],
                    net.line(step),
                    both(valid, ahead),
                )
                sends.append((ahead, one))
        share = net.copy(region, region, pair_sem, net.sibling(), valid)

        def action():
            if offset:
                net.arrival(region, line_sems.at[stage, z_from])
            for ahead, one in sends:
                guarded(ahead, one.start)
            share.start()

        guarded(valid, action)

    def attn_line(layer, part, offset):
        stage = layer * len(PARTS) + part
        along_line(
            stage,
            attn_piece(layer, part, q, core, z + offset),
            pair_attn_sems.at[stage],
            offset,
        )

    def attn_plane(layer, part, offset):
        stage = layer * len(PARTS) + part
        z_from = z + offset
        valid = in_line(offset)
        region = attn_piece(layer, part, q, core, z_from)
        sends = [
            net.copy(region, region, plane_sems.at[stage, q, z_from], net.peer(peer), valid)
            for peer in (net.first, net.second)
        ]

        def action():
            for one in sends:
                one.start()

        guarded(valid, action)

    def from_plane(layer, part, offset, which):
        stage = layer * len(PARTS) + part
        z_from = z + offset
        valid = in_line(offset)
        peer = (net.first, net.second, net.diagonal)[which]
        region = attn_piece(layer, part, peer, core, z_from)
        arrived = plane_sems.at[stage, peer, z_from]
        sends = []
        if which == 0:
            sends.append(net.copy(region, region, arrived, net.peer(net.second), valid))
        sends.append(
            net.copy(region, region, pair_attn_sems.at[stage], net.sibling(), valid)
        )

        def action():
            net.arrival(region, arrived)
            for one in sends:
                one.start()

        guarded(valid, action)

    def attn_pairs(layer, part):
        first_kind, last_kind = PARTS[part]
        net.arrival(
            full.at[layer, first_kind:last_kind, :, pl.ds((1 - core) * chips_z, chips_z)],
            pair_attn_sems.at[layer * len(PARTS) + part],
        )

    def exchange_columns(layer):
        for peer in (net.first, net.second, net.diagonal):
            for kind, ref in enumerate((wg_ref, wu_ref, wd_ref)):
                net.copy(
                    ref.at[layer, :, pl.ds(peer * width, width)],
                    full.at[layer, 4 + kind, q, here],
                    share_sems.at[layer, q],
                    net.peer(peer),
                ).start()

    def columns_here(layer):
        wait_local(layers * len(PARTS) + layer)
        for peer in (net.first, net.second, net.diagonal):
            net.arrival(full.at[layer, 4:7, peer, here], share_sems.at[layer, peer])

    def ffn_line(layer, part, offset):
        along_line(
            layers * len(PARTS) + layer * tile_count + part,
            ffn_piece(layer, part, core, z + offset),
            pair_ffn_sems.at[layer * tile_count + part],
            offset,
        )

    def ffn_pairs(layer, part):
        span = pl.ds(part * tile, tile)
        net.arrival(
            full.at[layer, 4:7, :, pl.ds((1 - core) * chips_z, chips_z), :, span],
            pair_ffn_sems.at[layer * tile_count + part],
        )

    def offsets(hops):
        return [hops, -hops] if hops else [0]

    def offsets(hops):
        return [hops, -hops] if hops else [0]

    chunk = 64 if rows % 64 == 0 else rows

    def embed():
        views = view_ids_ref.shape[1]
        per_view = rows // views
        half_width = width // 2
        place = lax.broadcasted_iota(jnp.int32, (1, half_width), 1).astype(jnp.float32)
        frequency = jnp.exp(-math.log(10000.0) * place / half_width)
        angles = time_ids_ref[z].astype(jnp.float32) * frequency
        code = jnp.concatenate([jnp.cos(angles), jnp.sin(angles)], axis=1)
        pose = lax.broadcasted_iota(jnp.int32, (table_ref.shape[0], 1), 0)
        for one in fetches:
            one.wait()
        groups = per_view // tokens_in.shape[1]
        for view in range(views):
            span = pl.ds(view * per_view, per_view)
            camera = jnp.sum(
                jnp.where(pose == view_ids_ref[z, view], table_in[...], 0.0),
                axis=0,
                keepdims=True,
            )
            part = tokens_in[view * groups : (view + 1) * groups].reshape(per_view, width)
            stream[span, :] = part.astype(jnp.float32) + (camera + code)

    def normalise(gain_ref, layer):
        def one(index, carry):
            span = pl.ds(pl.multiple_of(index * chunk, chunk), chunk)
            normed[0, span, :] = layer_norm(stream[span, :], gain_ref[layer : layer + 1, :])
            return carry

        lax.fori_loop(0, rows // chunk, one, 0)

    def weight(layer, kind, index, size):
        span = pl.ds(pl.multiple_of(index * size, size), size)
        return full[layer, kind, :, :, :, span].reshape(width, size)

    column = 256 if width % 256 == 0 else LANES

    def project(layer, kind):
        def one(index, carry):
            span = pl.ds(pl.multiple_of(index * column, column), column)
            staging[kind, :, span] = jnp.dot(
                normed[0], weight(layer, kind, index, column), preferred_element_type=jnp.float32
            ).astype(jnp.bfloat16)
            return carry

        lax.fori_loop(0, width // column, one, 0)

    window = head_window(head_size)

    def attend_heads(first_head, last_head):
        def one(head, carry):
            start = head * head_size
            base = pl.multiple_of(start // LANES * LANES, LANES)
            span = pl.ds(base, window)
            lane = lax.broadcasted_iota(jnp.int32, (1, window), 1) + base
            inside = jnp.logical_and(lane >= start, lane < start + head_size)
            query = staging[0, :, span]
            scores = out_terms(
                jnp.where(inside, query, jnp.zeros_like(query)), staging[1, :, span]
            ) * head_size ** (-0.5)
            peak = jnp.max(scores, axis=-1, keepdims=True)
            expons = jnp.exp(scores - peak)
            probs = (expons / jnp.sum(expons, axis=-1, keepdims=True)).astype(jnp.bfloat16)
            mixed = jnp.dot(
                probs, staging[2, :, span], preferred_element_type=jnp.float32
            ).astype(jnp.bfloat16)
            staging[0, :, span] = jnp.where(inside, mixed, query)
            return carry

        lax.fori_loop(first_head, last_head, one, 0)

    def project_out(layer):
        def one(index, carry):
            span = pl.ds(pl.multiple_of(index * column, column), column)
            stream[...] += out_terms(staging[0, :, span], weight(layer, 3, index, column))
            return carry

        lax.fori_loop(0, width // column, one, 0)

    half = rows // 2

    def ffn_tile(layer, part, unit):
        pair = pl.ds(unit % 2 * 2, 2)
        span = pl.ds(pl.multiple_of(unit // 2 * half, half), half)
        acts = normed[pair, span, :].reshape(2 * half, width)
        gate = jnp.dot(acts, weight(layer, 4, part, tile), preferred_element_type=jnp.float32)
        up = jnp.dot(acts, weight(layer, 5, part, tile), preferred_element_type=jnp.float32)
        gate = 0.5 * gate * (1.0 + lax.erf(gate * math.sqrt(0.5)))
        hidden = (gate * up).astype(jnp.bfloat16)
        term = out_terms(hidden, weight(layer, 6, part, tile)).reshape(2, half, width)
        if part == 0:
            total[pair, span, :] = term
        else:
            total[pair, span, :] = total[pair, span, :] + term

    def head_of(part):
        count = D // head_size
        return count * part // 2

    rows_sent, terms_sent = [], []

    def half_span(index):
        return pl.ds(index * half, half)

    def send_rows(layer, index, role, target, side):
        span = half_span(index)
        rows_sent.append(
            net.copy(
                normed.at[SLOTS[role], span],
                normed.at[SLOTS[target], span],
                rows_sems.at[layer, index, target - 1],
                net.peer((net.first, net.second)[side]),
                later=False,
            )
        )
        rows_sent[-1].start()

    def rows_arrival(layer, index, role):
        net.arrival(
            normed.at[SLOTS[role], half_span(index)], rows_sems.at[layer, index, role - 1]
        )

    def term_arrival(layer, index, target):
        net.arrival(
            landing.at[target, half_span(index)], term_sems.at[layer, index, target]
        )

    def send_term(layer, index, target):
        span = half_span(index)
        role = (3, 1, 2)[target]
        value = total[SLOTS[role], span, :]
        if target == 2:
            term_arrival(layer, index, 0)
            value = value + landing[0, span, :].astype(jnp.float32)
        staging[target, span, :] = value.astype(jnp.bfloat16)
        terms_sent.append(
            net.copy(
                staging.at[target, span],
                landing.at[target, span],
                term_sems.at[layer, index, target],
                net.peer((net.first, net.first, net.second)[target]),
                later=False,
            )
        )
        terms_sent[-1].start()

    def settle(copies):
        for one in copies:
            one.wait_send()
        copies.clear()

    def residual(layer):
        last_layer = layer == layers - 1

        def add(index, carry):
            span = pl.ds(pl.multiple_of(index * chunk, chunk), chunk)
            summed = stream[span, :] + (
                total[SLOTS[0], span, :]
                + landing[1, span, :].astype(jnp.float32)
                + landing[2, span, :].astype(jnp.float32)
            )
            if last_layer:
                out_ref[span, :] = summed.astype(out_ref.dtype)
            else:
                stream[span, :] = summed
            return carry

        lax.fori_loop(0, rows // chunk, add, 0)
        settle(terms_sent)

    def piece(kind, layer, part, hops):
        if kind == ATTN:
            if hops == 0:
                wait_local(layer * len(PARTS) + part)
            for offset in offsets(hops):
                attn_line(layer, part, offset)
        else:
            if hops == 0 and part == 0:
                columns_here(layer)
            for offset in offsets(hops):
                ffn_line(layer, part, offset)

    def tiles(layer, part, first_unit, last_unit):
        if last_unit - first_unit == 1:
            ffn_tile(layer, part, first_unit)
            return

        def one(unit, carry):
            ffn_tile(layer, part, unit)
            return carry

        lax.fori_loop(first_unit, last_unit, one, 0)

    def run(token):
        name, rest = token[0], token[1:]
        if name == LINE:
            piece(*rest)
        elif name == OUT:
            for offset in offsets(rest[2]):
                attn_plane(rest[0], rest[1], offset)
        elif name == NEAR:
            for offset in offsets(rest[2]):
                from_plane(rest[0], rest[1], offset, 0)
                from_plane(rest[0], rest[1], offset, 1)
        elif name == FAR:
            for offset in offsets(rest[2]):
                from_plane(rest[0], rest[1], offset, 2)
        elif name == COLUMNS:
            exchange_columns(rest[0])
        elif name == PAIRS_ATTN:
            attn_pairs(*rest)
        elif name == PAIRS_FFN:
            ffn_pairs(*rest)
        elif name == EMBED:
            embed()
        elif name == NORM:
            normalise((gain_attn_ref, gain_ffn_ref)[rest[1]], rest[0])
        elif name == PROJECT:
            project(*rest)
        elif name == MIX:
            attend_heads(head_of(rest[1]), head_of(rest[1] + 1))
        elif name == PROJECT_OUT:
            project_out(rest[0])
        elif name == ROWS_OUT:
            send_rows(rest[0], rest[1], 0, 1, 0)
            send_rows(rest[0], rest[1], 0, 2, 1)
        elif name == ROWS_ON:
            rows_arrival(rest[0], rest[1], 1)
            send_rows(rest[0], rest[1], 1, 3, 1)
        elif name == ROWS_IN:
            rows_arrival(*rest)
        elif name == ROWS_DONE:
            settle(rows_sent)
        elif name == TILES:
            tiles(*rest)
        elif name == TERM:
            send_term(*rest)
        elif name == TERM_IN:
            term_arrival(*rest)
        elif name == RESIDUAL:
            residual(rest[0])

    for token in schedule(chips_z, layers, tile_count):
        run(token)
    for condition, action in net.finish:
        guarded(condition, action)


def merged(tokens):
    out = []
    for token in tokens:
        if token[0] == TILES:
            layer, part, index, first_pair, count = token[1:]
            first = 2 * index + first_pair
            token = (TILES, layer, part, first, first + count)
            previous = out[-1]
            if previous[:3] == token[:3] and previous[4] == first:
                out[-1] = previous[:4] + (first + count,)
                continue
        out.append(token)
    return out


def schedule(chips_z, layers, tile_count):
    if (chips_z, layers, tile_count) == (4, 2, 5):
        return merged(ORDER)
    return merged(plain_schedule(chips_z, layers, tile_count))


def plain_schedule(chips_z, layers, tile_count):
    tokens = [(COLUMNS, 0), (EMBED,), (NORM, 0, 0)]
    for layer in range(layers):
        if layer:
            tokens.append((COLUMNS, layer))
        for part in range(len(PARTS)):
            for hops in range(chips_z):
                tokens += [(LINE, ATTN, layer, part, hops), (OUT, layer, part, hops)]
                tokens += [(NEAR, layer, part, hops), (FAR, layer, part, hops)]
            tokens.append((PAIRS_ATTN, layer, part))
        if layer:
            tokens.append((NORM, layer, 0))
        tokens += [(PROJECT, layer, kind) for kind in range(3)]
        tokens += [(MIX, layer, 0), (MIX, layer, 1), (PROJECT_OUT, layer)]
        tokens.append((NORM, layer, 1))
        tokens += [(ROWS_OUT, layer, 0), (ROWS_OUT, layer, 1)]
        for index in range(2):
            tokens += [(ROWS_ON, layer, index), (ROWS_IN, layer, index, 2)]
            tokens.append((ROWS_IN, layer, index, 3))
        for part in range(tile_count):
            tokens += [(LINE, FFN, layer, part, hops) for hops in range(chips_z)]
            tokens.append((PAIRS_FFN, layer, part))
            tokens += [(TILES, layer, part, index, 0, 2) for index in range(2)]
        tokens.append((ROWS_DONE, layer))
        for target in range(3):
            tokens += [(TERM, layer, index, target) for index in range(2)]
        for target in (1, 2):
            tokens += [(TERM_IN, layer, index, target) for index in range(2)]
        tokens.append((RESIDUAL, layer))
    return tokens


ORDER = (
    (LINE, ATTN, 0, 0, 0), (LINE, ATTN, 1, 0, 0), (LINE, ATTN, 0, 1, 0), (OUT, 0, 1, 0),
    (COLUMNS, 0), (LINE, ATTN, 0, 0, 1), (OUT, 0, 0, 0), (LINE, ATTN, 1, 1, 0),
    (LINE, ATTN, 0, 1, 1), (OUT, 0, 0, 1), (LINE, ATTN, 1, 0, 1), (LINE, ATTN, 0, 0, 2),
    (OUT, 0, 0, 2), (OUT, 0, 1, 1), (LINE, ATTN, 0, 1, 2), (EMBED,), (NEAR, 0, 0, 1),
    (OUT, 0, 1, 2), (LINE, ATTN, 1, 1, 1), (LINE, FFN, 0, 0, 0), (OUT, 1, 0, 0),
    (LINE, ATTN, 0, 0, 3), (LINE, FFN, 0, 1, 0), (LINE, ATTN, 0, 1, 3), (OUT, 0, 0, 3),
    (LINE, ATTN, 1, 0, 2), (NEAR, 0, 1, 2), (LINE, FFN, 0, 0, 1), (NEAR, 0, 0, 3),
    (OUT, 0, 1, 3), (NEAR, 0, 0, 0), (NEAR, 0, 0, 2), (LINE, FFN, 0, 1, 1), (LINE, FFN, 0, 0, 2),
    (NEAR, 0, 1, 0), (FAR, 0, 0, 0), (NEAR, 0, 1, 1), (NEAR, 0, 1, 3), (NEAR, 1, 0, 0),
    (NORM, 0, 0), (FAR, 0, 0, 1), (COLUMNS, 1), (OUT, 1, 1, 0), (LINE, FFN, 0, 4, 0),
    (OUT, 1, 0, 1), (FAR, 0, 1, 0), (LINE, ATTN, 1, 1, 2), (FAR, 0, 1, 2), (LINE, FFN, 0, 2, 0),
    (FAR, 0, 0, 3), (FAR, 0, 0, 2), (PAIRS_ATTN, 0, 0), (LINE, ATTN, 1, 0, 3), (PROJECT, 0, 0),
    (PROJECT, 0, 1), (FAR, 0, 1, 3), (PROJECT, 0, 2), (FAR, 0, 1, 1), (MIX, 0, 0), (MIX, 0, 1),
    (PAIRS_ATTN, 0, 1), (LINE, FFN, 0, 4, 1), (OUT, 1, 0, 3), (LINE, FFN, 0, 3, 0),
    (PROJECT_OUT, 0), (NORM, 0, 1), (LINE, FFN, 0, 2, 1), (LINE, FFN, 0, 0, 3),
    (LINE, FFN, 0, 4, 2), (ROWS_OUT, 0, 0), (PAIRS_FFN, 0, 0), (LINE, FFN, 0, 3, 1),
    (LINE, ATTN, 1, 1, 3), (ROWS_OUT, 0, 1), (LINE, FFN, 0, 2, 2), (ROWS_ON, 0, 1),
    (LINE, FFN, 0, 1, 2), (ROWS_ON, 0, 0), (ROWS_IN, 0, 1, 3), (LINE, FFN, 0, 2, 3),
    (NEAR, 1, 0, 3), (LINE, FFN, 0, 1, 3), (ROWS_IN, 0, 1, 2), (OUT, 1, 0, 2),
    (LINE, FFN, 0, 3, 2), (LINE, FFN, 1, 0, 0), (TILES, 0, 0, 1, 0, 2), (PAIRS_FFN, 0, 2),
    (ROWS_IN, 0, 0, 3), (LINE, FFN, 0, 4, 3), (NEAR, 1, 0, 1), (LINE, FFN, 1, 1, 0),
    (ROWS_IN, 0, 0, 2), (PAIRS_FFN, 0, 1), (FAR, 1, 0, 0), (LINE, FFN, 1, 2, 0),
    (LINE, FFN, 1, 3, 0), (FAR, 1, 0, 3), (TILES, 0, 0, 0, 0, 2), (ROWS_DONE, 0),
    (LINE, FFN, 1, 4, 0), (OUT, 1, 1, 2), (TILES, 0, 1, 0, 0, 2), (PAIRS_FFN, 0, 4),
    (TILES, 0, 1, 1, 0, 2), (LINE, FFN, 0, 3, 3), (NEAR, 1, 0, 2), (TILES, 0, 2, 1, 0, 2),
    (PAIRS_FFN, 0, 3), (OUT, 1, 1, 3), (TILES, 0, 3, 1, 0, 2), (TILES, 0, 4, 1, 1, 1),
    (FAR, 1, 0, 1), (TERM, 0, 1, 1), (TERM, 0, 1, 0), (TILES, 0, 2, 0, 0, 2),
    (TILES, 0, 3, 0, 0, 2), (TILES, 0, 4, 0, 1, 1), (TILES, 0, 4, 1, 0, 1), (TERM, 0, 0, 0),
    (NEAR, 1, 1, 0), (NEAR, 1, 1, 3), (LINE, FFN, 1, 2, 1), (TILES, 0, 4, 0, 0, 1),
    (FAR, 1, 0, 2), (TERM, 0, 1, 2), (LINE, FFN, 1, 0, 1), (TERM, 0, 0, 2), (TERM, 0, 0, 1),
    (TERM_IN, 0, 1, 1), (LINE, FFN, 1, 1, 1), (OUT, 1, 1, 1), (TERM_IN, 0, 0, 2),
    (TERM_IN, 0, 0, 1), (TERM_IN, 0, 1, 2), (FAR, 1, 1, 3), (LINE, FFN, 1, 4, 1),
    (PAIRS_ATTN, 1, 0), (LINE, FFN, 1, 3, 1), (RESIDUAL, 0), (NORM, 1, 0), (NEAR, 1, 1, 2),
    (PROJECT, 1, 0), (NEAR, 1, 1, 1), (LINE, FFN, 1, 0, 2), (PROJECT, 1, 1), (FAR, 1, 1, 0),
    (FAR, 1, 1, 2), (LINE, FFN, 1, 2, 2), (PROJECT, 1, 2), (FAR, 1, 1, 1), (MIX, 1, 0),
    (MIX, 1, 1), (PAIRS_ATTN, 1, 1), (PROJECT_OUT, 1), (NORM, 1, 1), (ROWS_OUT, 1, 0),
    (LINE, FFN, 1, 1, 2), (LINE, FFN, 1, 3, 2), (LINE, FFN, 1, 2, 3), (ROWS_ON, 1, 0),
    (ROWS_OUT, 1, 1), (LINE, FFN, 1, 0, 3), (PAIRS_FFN, 1, 0), (ROWS_IN, 1, 0, 3),
    (LINE, FFN, 1, 1, 3), (LINE, FFN, 1, 4, 2), (PAIRS_FFN, 1, 2), (ROWS_IN, 1, 0, 2),
    (TILES, 1, 0, 0, 0, 2), (ROWS_ON, 1, 1), (LINE, FFN, 1, 3, 3), (PAIRS_FFN, 1, 1),
    (TILES, 1, 1, 0, 0, 2), (TILES, 1, 2, 0, 0, 2), (ROWS_IN, 1, 1, 2), (LINE, FFN, 1, 4, 3),
    (PAIRS_FFN, 1, 3), (TILES, 1, 3, 0, 0, 2), (PAIRS_FFN, 1, 4), (TILES, 1, 4, 0, 1, 1),
    (ROWS_IN, 1, 1, 3), (ROWS_DONE, 1), (TERM, 1, 0, 0), (TILES, 1, 0, 1, 0, 2),
    (TILES, 1, 4, 0, 0, 1), (TERM, 1, 0, 1), (TILES, 1, 1, 1, 0, 2), (TILES, 1, 2, 1, 0, 2),
    (TERM, 1, 0, 2), (TILES, 1, 3, 1, 0, 2), (TILES, 1, 4, 1, 1, 1), (TERM, 1, 1, 0),
    (TILES, 1, 4, 1, 0, 1), (TERM, 1, 1, 1), (TERM, 1, 1, 2), (TERM_IN, 1, 1, 2),
    (TERM_IN, 1, 0, 1), (TERM_IN, 1, 1, 1), (TERM_IN, 1, 0, 2), (RESIDUAL, 1),
)


def head_window(head_size):
    reach = head_size + LANES - math.gcd(head_size, LANES)
    return -(-reach // LANES) * LANES


def fused_blocks(tokens, view_ids, time_ids, camera_table, norm_attn, norm_ffn, shards, chips_z):
    layers, share, width = shards[0].shape
    inner = shards[4].shape[2]
    tile = 256 if width % 256 == 0 else LANES
    tile_count = width // tile
    rows = tokens.shape[0]
    head_size = D // HEADS
    stages = layers * (len(PARTS) + tile_count)
    shape = (layers, chips_z, width, tile, tile_count, head_size)
    anywhere = pl.BlockSpec(memory_space=pl.ANY)
    inside = pl.BlockSpec(memory_space=pltpu.VMEM)
    scalars = pl.BlockSpec(memory_space=pltpu.SMEM)
    kind = tokens.dtype
    return pl.pallas_call(
        functools.partial(fused_kernel, shape),
        out_shape=jax.ShapeDtypeStruct((rows, width), kind),
        in_specs=[anywhere, scalars, scalars, anywhere] + [inside] * 2 + [anywhere] * 7,
        out_specs=inside,
        scratch_shapes=[
            pltpu.VMEM((layers, 7, PLANE, 2 * chips_z, share, width), kind),
            pltpu.VMEM((PLANE, rows, width), kind),
            pltpu.VMEM((3, rows, width), kind),
            pltpu.VMEM((3, rows, width), kind),
            pltpu.VMEM((PLANE, rows, width), jnp.float32),
            pltpu.VMEM((rows, width), jnp.float32),
            pltpu.VMEM((rows // 8, 8, width), kind),
            pltpu.VMEM(camera_table.shape, camera_table.dtype),
            pltpu.SemaphoreType.DMA((layers * 7,)),
            pltpu.SemaphoreType.DMA((2,)),
            pltpu.SemaphoreType.DMA((POOL + NAMED,)),
            pltpu.SemaphoreType.DMA((stages, chips_z)),
            pltpu.SemaphoreType.DMA((layers * len(PARTS), PLANE, chips_z)),
            pltpu.SemaphoreType.DMA((layers, PLANE)),
            pltpu.SemaphoreType.DMA((layers * len(PARTS),)),
            pltpu.SemaphoreType.DMA((layers * tile_count,)),
            pltpu.SemaphoreType.DMA((layers, 2, 3)),
            pltpu.SemaphoreType.DMA((layers, 2, 3)),
        ],
        compiler_params=pltpu.CompilerParams(
            collective_id=0, has_side_effects=True, vmem_limit_bytes=67_000_000
        ),
        name="fused_blocks",
    )(
        tokens.reshape(rows // 8, 8, width),
        view_ids,
        time_ids,
        camera_table,
        norm_attn,
        norm_ffn,
        *shards,
    )


def attend(packed, head_size):
    total_rows = packed.shape[0]
    width = packed.shape[1] // 3
    set_rows = VIEWS * HW
    query_rows, sources = packed[:, :width], packed[:, width:]
    if total_rows % set_rows != 0:
        first = lax.axis_index("tp") * total_rows // set_rows * set_rows
        sources = lax.all_gather(sources, "tp", axis=0, tiled=True)
        sources = lax.dynamic_slice_in_dim(sources, first, set_rows, 0)
    set_count = sources.shape[0] // set_rows
    query_rows = query_rows.reshape(set_count, -1, width // head_size, head_size)
    key_rows = sources[:, :width].reshape(set_count, set_rows, -1, head_size)
    value_rows = sources[:, width:].reshape(set_count, set_rows, -1, head_size)
    scores = jnp.einsum(
        "bqhd,bkhd->bhqk", query_rows, key_rows, preferred_element_type=jnp.float32
    ) * head_size ** (-0.5)
    peak = jnp.max(scores, axis=-1, keepdims=True)
    expons = jnp.exp(scores - peak)
    attn_probs = (expons / jnp.sum(expons, axis=-1, keepdims=True)).astype(jnp.bfloat16)
    mixed_rows = jnp.einsum(
        "bhqk,bkhd->bqhd", attn_probs, value_rows, preferred_element_type=jnp.float32
    )
    return mixed_rows.astype(jnp.bfloat16).reshape(total_rows, width)


def out_terms(mixed_rows, weight):
    return lax.dot_general(
        mixed_rows, weight, (((1,), (1,)), ((), ())), preferred_element_type=jnp.float32
    )


def body(
    tokens,
    view_ids,
    time_ids,
    camera_table,
    norm_attn,
    norm_ffn,
    w_query,
    w_key,
    w_value,
    w_out,
    w_gate,
    w_up,
    w_down,
):
    tp_count = lax.axis_size("tp")
    rep_count = lax.axis_size("rep")
    width = w_query.shape[2]
    inner = w_gate.shape[2]
    head_size = D // HEADS
    shards = (w_query, w_key, w_value, w_out, w_gate, w_up, w_down)
    share_rows = tokens.shape[0]
    fits = (
        rep_count == 2 * PLANE
        and share_rows == VIEWS * HW
        and time_ids.shape[0] == tp_count
        and inner == PLANE * width
        and w_query.shape[1] % 8 == 0
        and share_rows % 32 == 0
    )
    if fits:
        return fused_blocks(
            tokens, view_ids, time_ids, camera_table, norm_attn, norm_ffn, shards, tp_count
        )

    row_ids = lax.axis_index("tp") * share_rows + jnp.arange(share_rows, dtype=jnp.int32)
    stream = tokens.astype(jnp.float32) + conditioning(row_ids, view_ids, time_ids, camera_table)

    def whole_weight(layer_index, first, count, after):
        own = [shard[layer_index] for shard in shards[first : first + count]]
        own, _ = lax.optimization_barrier((own, after))
        return lax.all_gather(jnp.concatenate(own, axis=1), ("rep", "tp"), axis=0, tiled=True)

    for layer_index in range(LAYERS):
        normed = layer_norm(stream, norm_attn[layer_index])
        qkv_w = whole_weight(layer_index, 0, 3, normed)
        packed = jnp.dot(normed, qkv_w, preferred_element_type=jnp.float32).astype(jnp.bfloat16)
        mixed_rows = attend(packed, head_size)
        stream = stream + out_terms(mixed_rows, whole_weight(layer_index, 3, 1, mixed_rows))
        normed = layer_norm(stream, norm_ffn[layer_index])
        gate_w = whole_weight(layer_index, 4, 1, normed)
        gate_part = jnp.dot(normed, gate_w, preferred_element_type=jnp.float32)
        up_w = whole_weight(layer_index, 5, 1, gate_part)
        up_part = jnp.dot(normed, up_w, preferred_element_type=jnp.float32)
        hidden = (jax.nn.gelu(gate_part, approximate=False) * up_part).astype(jnp.bfloat16)
        stream = stream + out_terms(hidden, whole_weight(layer_index, 6, 1, hidden))
    return stream.astype(jnp.bfloat16)


def solution(mesh):
    return jax.shard_map(
        body,
        mesh=mesh,
        in_specs=(
            P(("rep", "tp"), None),
            P("rep", None),
            P("rep"),
            P(),
            P(),
            P(),
            P(None, ("rep", "tp"), None),
            P(None, ("rep", "tp"), None),
            P(None, ("rep", "tp"), None),
            P(None, ("rep", "tp"), None),
            P(None, ("rep", "tp"), None),
            P(None, ("rep", "tp"), None),
            P(None, ("rep", "tp"), None),
        ),
        out_specs=P(("rep", "tp"), None),
        check_vma=False,
    )
```
